256 devices in a mesh: pb: 2 (over y), col: 32 (over z, core), row: 4 (over x).
Axes of the slice: x: 4, y: 2, z: 16, core: 2. Of those that a mesh axis runs over, the one named last changes fastest.
The devices are a block of a 4x16x16 slice.
Arguments:
- pair_density: bfloat16 [6144, 6144], P(('pb', 'col'), 'row'), parts along dimension 0, may hold values from -0.19921875 to 0.19921875
- band_pairs: int32 [2, 3072], replicated, may hold values from 0 to 255, as said below
- valence: float32 [256], replicated, may hold values from -12 to -2
- conduction: float32 [12], replicated, may hold values from 1 to 8
- wave_vectors: int32 [3, 12288], P(None, 'pb'), parts along dimension 1, may hold values from -6 to 6
- momentum: float32 [6], P('pb'), parts along dimension 0, may hold values from 0.3 to 0.7
- guess_scale: float32 [12288], P('pb'), parts along dimension 0, may hold values from 0.4 to 0.75
Outputs:
- epsilon: float32 [12288, 6144], P(('pb', 'row'), 'col'), parts along dimension 0
- inverse: float32 [12288, 6144], P(('pb', 'row'), 'col'), parts along dimension 0
The draws below stay inside these ranges and needn't reach their ends.
There are 2 independent parts, one for each index of `pb`. The reference program is written for one: setup_inputs(seed, part) draws one part's arguments, and reference() takes and returns one part's arrays. A program takes and returns all parts, laid end to end along the dimension named above; an argument that names none is the same for every part. Nothing has to cross between parts.
Inputs may be any that keep to these rules, and one draw needn't show every extreme that they name: `band_pairs`: column p names a valence band below 256 in row 0 and a conduction band below 12 in row 1; every such pair of bands appears in exactly one column.
All inputs are finite; a program needn't handle non-finite values.
Results may differ from the reference program's by a relative error of at most 0.0036.
The reference program's roundings to bfloat16 on the way (of `weighted`, `mixed_b` and `square_b`) count: a program that leaves them out, or rounds other values in their place, can miss the bound.
Values may be sent and summed in bfloat16 or wider, within the bound.
A program may use at most 64 MiB of HBM per device.

```python
import math
import jax
import jax.numpy as jnp
from jax import lax

NG = 6144
NV = 256
NC = 12
PAIRS = 3072


def draw_band_pairs(key, part):
    shuffled = jax.random.permutation(jax.random.fold_in(key, 17), NV * NC).astype(jnp.int32)
    return jnp.stack([shuffled // NC, shuffled % NC]).astype(jnp.int32)


def place_ends(result, stream_key, low, high):
    longest = result.shape.index(max(result.shape))
    spots = []
    for shift in (0, 1):
        where = [jax.random.randint(jax.random.fold_in(stream_key, axis), (), 0, length) for axis, length in enumerate(result.shape)]
        where[longest] = (where[longest] + shift) % result.shape[longest]
        spots.append(tuple(where))
    return result.at[spots[0]].set(low).at[spots[1]].set(high)


def spiked(array, key, source, target, parts, factor):
    owner, partner = [(jnp.arange(array.shape[position]) // (array.shape[position] // parts)).reshape([-1 if axis == position else 1 for axis in range(array.ndim)]) for position in (source, target)]
    chosen = jax.random.permutation(key, parts)[partner]
    strong = (owner == chosen) | (owner == (partner + parts // 2) % parts)
    return jnp.where(strong, factor * array, array)


def levels(stream_key, extent, pieces, low, high):
    gain, own = 1.0, jax.random.fold_in(stream_key, 6)
    for position, shards_of in pieces:
        steps = jnp.exp(jax.random.uniform(jax.random.fold_in(own, position), (shards_of,), jnp.float32, low / len(pieces), high / len(pieces)))
        gain = gain * jnp.repeat(steps, extent[position] // shards_of).reshape([-1 if axis == position else 1 for axis in range(len(extent))])
    return gain


def noise_with(rng, dims, deviation, reach, pieces, heavy, kind=jnp.bfloat16):
    result = deviation * jax.random.normal(rng, dims, jnp.float32)
    if pieces:
        result = result * levels(rng, dims, pieces, -0.22, 0.18)
    return jnp.clip(spiked(result, jax.random.fold_in(rng, 3), *heavy), -reach, reach).astype(kind)


def setup_inputs(seed: int = 0, part: int = 0) -> dict:
    keys = jax.random.split(jax.random.key(seed), 8)
    own_keys = jax.random.split(jax.random.fold_in(keys[7], part), 8)
    pair_density = noise_with(own_keys[0], (PAIRS, NG), 0.033, 0.19921875, ((0, 32), (1, 4)), (0, 1, 32, 2.75))
    band_pairs = draw_band_pairs(jax.random.fold_in(keys[7], 71), part)
    valence = jnp.clip(jax.random.uniform(keys[2], (NV,), jnp.float32, -12.0, -2.0), -12.0, -2.0)
    conduction = jnp.clip(jax.random.uniform(keys[3], (NC,), jnp.float32, 1.0, 8.0), 1.0, 8.0)
    wave_vectors = place_ends(jax.random.randint(own_keys[4], (3, NG), -6, 7), jax.random.fold_in(own_keys[4], 1), -6, 6).astype(jnp.int32)
    momentum = jnp.clip(jax.random.uniform(own_keys[5], (3,), jnp.float32, 0.3, 0.7), 0.3, 0.7)
    guess_scale = jnp.clip(jax.random.uniform(own_keys[6], (NG,), jnp.float32, 0.4, 0.75), 0.4, 0.75)
    return dict(pair_density=pair_density, band_pairs=band_pairs, valence=valence, conduction=conduction, wave_vectors=wave_vectors, momentum=momentum, guess_scale=guess_scale)


def reference(pair_density, band_pairs, valence, conduction, wave_vectors, momentum, guess_scale):
    shifted = wave_vectors.astype(jnp.float32) + momentum[:, None]
    squared_norm = lax.optimization_barrier(jnp.sum(shifted * shifted, axis=0))
    sqrt_v = jnp.sqrt(4.0 * math.pi / squared_norm)
    valence_of = valence[band_pairs[0].astype(jnp.int32)]
    conduction_of = conduction[band_pairs[1].astype(jnp.int32)]
    weight = 4.0 / (valence_of - conduction_of)
    weighted = (weight[:, None] * pair_density.astype(jnp.float32)).astype(jnp.bfloat16)
    chi_zero = jnp.dot(weighted.T, pair_density, preferred_element_type=jnp.float32)
    identity = jnp.eye(chi_zero.shape[0], dtype=jnp.float32)
    epsilon = identity - sqrt_v[:, None] * chi_zero * sqrt_v[None, :]
    guess = guess_scale / jnp.diagonal(epsilon)
    mixed = epsilon * guess[None, :]
    mixed_b = mixed.astype(jnp.bfloat16)
    square = jnp.dot(mixed_b, mixed_b, preferred_element_type=jnp.float32)
    square_b = square.astype(jnp.bfloat16)
    cube = jnp.dot(mixed_b, square_b, preferred_element_type=jnp.float32)
    inverse = guess[:, None] * (4.0 * identity - 6.0 * mixed + 4.0 * square - cube)
    return (epsilon, inverse)
```

```python
import math

import jax
import jax.numpy as jnp
from jax import lax
from jax.sharding import PartitionSpec as P


def lookup(indices, table):
    levels = jnp.arange(table.shape[0], dtype=jnp.int32)
    picked = indices[:, None] == levels[None, :]
    return jnp.sum(jnp.where(picked, table[None, :], 0.0), axis=1)


def on_device(pair_density, band_pairs, valence, conduction, wave_vectors, momentum, guess_scale):
    column_index = lax.axis_index("col")
    row_index = lax.axis_index("row")
    row_height = pair_density.shape[1]
    whole_width = row_height * lax.axis_size("row")
    strip_width = whole_width // lax.axis_size("col")
    valence_of = lookup(band_pairs[0], valence)
    conduction_of = lookup(band_pairs[1], conduction)
    weight = 4.0 / (valence_of - conduction_of)
    shifted = wave_vectors.astype(jnp.float32) + momentum[:, None]
    sqrt_all = jnp.sqrt(4.0 * math.pi / jnp.sum(shifted * shifted, axis=0))
    row_first = row_index * row_height
    column_first = column_index * strip_width
    sqrt_rows = lax.dynamic_slice_in_dim(sqrt_all, row_first, row_height, 0)
    sqrt_cols = lax.dynamic_slice_in_dim(sqrt_all, column_first, strip_width, 0)
    scale_rows = lax.dynamic_slice_in_dim(guess_scale, row_first, row_height, 0)
    scale_cols = lax.dynamic_slice_in_dim(guess_scale, column_first, strip_width, 0)
    panel_pairs = lax.all_gather(pair_density, "col", axis=0, tiled=True)
    owner = column_first // row_height
    offset = column_first % row_height
    own_slice = lax.dynamic_slice_in_dim(panel_pairs, offset, strip_width, 1)
    candidates = lax.all_gather(own_slice, "row", axis=1, tiled=True)
    strip_pairs = lax.dynamic_slice_in_dim(candidates, owner * strip_width, strip_width, 1)
    weighted = (weight[:, None] * panel_pairs.astype(jnp.float32)).astype(jnp.bfloat16)
    weighted_strip = (weight[:, None] * strip_pairs.astype(jnp.float32)).astype(jnp.bfloat16)
    chi_block = lax.dot_general(
        weighted, strip_pairs, (((0,), (0,)), ((), ())), preferred_element_type=jnp.float32
    )
    chi_rows = jnp.sum(weighted.astype(jnp.float32) * panel_pairs.astype(jnp.float32), axis=0)
    chi_cols = jnp.sum(weighted_strip.astype(jnp.float32) * strip_pairs.astype(jnp.float32), axis=0)
    global_rows = row_first + jnp.arange(row_height, dtype=jnp.int32)
    global_cols = column_first + jnp.arange(strip_width, dtype=jnp.int32)
    identity = (global_rows[:, None] == global_cols[None, :]).astype(jnp.float32)
    epsilon = identity - sqrt_rows[:, None] * chi_block * sqrt_cols[None, :]
    diagonal_rows = 1.0 - sqrt_rows * chi_rows * sqrt_rows
    guess_rows = scale_rows / diagonal_rows
    guess_cols = scale_cols / (1.0 - sqrt_cols * chi_cols * sqrt_cols)
    mixed = epsilon * guess_cols[None, :]
    mixed_b = mixed.astype(jnp.bfloat16)
    mixed_diagonal = diagonal_rows * guess_rows
    rounded_diagonal = mixed_diagonal.astype(jnp.bfloat16).astype(jnp.float32)
    delta = guess_rows + (rounded_diagonal - mixed_diagonal)
    inner = sqrt_rows * guess_rows

    def times_mixed(block):
        wide = block.astype(jnp.float32)
        scaled = (inner[:, None] * wide).astype(jnp.bfloat16)
        partial = jnp.dot(panel_pairs, scaled, preferred_element_type=jnp.float32)
        total = lax.psum(partial.astype(jnp.bfloat16), "row")
        spread = lax.dot_general(
            weighted, total, (((0,), (0,)), ((), ())), preferred_element_type=jnp.float32
        )
        return delta[:, None] * wide - sqrt_rows[:, None] * spread

    square = times_mixed(mixed_b)
    cube = times_mixed(square.astype(jnp.bfloat16))
    inverse = guess_rows[:, None] * (4.0 * identity - 6.0 * mixed + 4.0 * square - cube)
    return (epsilon, inverse)


def solution(mesh):
    placed = (P(("pb", "col"), "row"), P(), P(), P(), P(None, "pb"), P("pb"), P("pb"))
    return jax.shard_map(
        on_device,
        mesh=mesh,
        in_specs=placed,
        out_specs=(P(("pb", "row"), "col"), P(("pb", "row"), "col")),
        check_vma=False,
    )
```

```python
import functools
import math

import jax
import jax.numpy as jnp
from jax import lax
from jax.experimental import pallas as pl
from jax.experimental.pallas import tpu as pltpu
from jax.sharding import PartitionSpec as P

MESH = pl.DeviceIdType.MESH
BF = jnp.bfloat16
F32 = jnp.float32
SUBS = 2


def lookup(indices, table):
    levels = jnp.arange(table.shape[0], dtype=jnp.int32)
    picked = indices[:, None] == levels[None, :]
    return jnp.sum(jnp.where(picked, table[None, :], 0.0), axis=1)


def mm(a, b, dims):
    return lax.dot_general(a, b, (dims, ((), ())), preferred_element_type=F32)


def kernel(ncol, nrow, pd, weights, rowv, colv, eps_out, inv_out,
           panel, wpan, strip, acc, chir, chic, rvec, cvec, sbuf, mixb, square, ybuf,
           keep, qsend, qrecv, qfull,
           ring_s, ring_r, pair_s, pair_r, sx_s, sx_r, sp_s, sp_r, own_s, loc_s, x_s, x_r):
    nz = ncol // 2
    half = nz // 2
    per = nz // nrow
    ch, height = pd.shape
    sub = ch // SUBS
    chip_wide = strip.shape[2]
    wide = chip_wide // 2
    hj = wide // 2
    pp = keep.shape[3]
    cpp = pp // ch
    col = lax.axis_index("col")
    x = lax.axis_index("row")
    z = col // 2
    core = lax.rem(col, 2)
    xr, xl = lax.rem(x + 1, nrow), lax.rem(x + nrow - 1, nrow)
    x2 = lax.rem(x + 2, nrow)
    up, down = lax.rem(col + 2, ncol), lax.rem(col + ncol - 2, ncol)
    mate = col + 1 - 2 * core
    home = z // per
    dist = lax.rem(x - home + nrow, nrow)
    lane0 = pl.multiple_of(lax.rem(z, per) * chip_wide, 128)

    def to(src, dst, ssem, rsem, **where):
        return pltpu.make_async_remote_copy(
            src_ref=src, dst_ref=dst, send_sem=ssem, recv_sem=rsem,
            device_id=where, device_id_type=MESH)

    barrier = pltpu.get_barrier_semaphore()
    for where in (dict(col=up), dict(col=down), dict(col=mate), dict(row=xr), dict(row=xl)):
        pl.semaphore_signal(barrier, inc=1, device_id=where, device_id_type=MESH)
    pl.semaphore_wait(barrier, 5)

    def chunk_of(d, s):
        away = jnp.where(d == 0, nz - s, s)
        return 2 * lax.rem(z + away, nz) + core

    def piece(ref, k, j):
        return ref.at[k, pl.ds(j * sub, sub)]

    def ring(d, s, j):
        k = chunk_of(d, s - 1)
        src = piece(panel, k, j)
        return to(src, piece(panel, k, j), ring_s.at[d, s - 1, j], ring_r.at[d, s - 1, j],
                  col=up if d == 0 else down)

    def ring_in(d, s, j):
        k = chunk_of(d, s)
        return to(piece(panel, k, j), piece(panel, k, j), ring_s.at[d, s - 1, j],
                  ring_r.at[d, s - 1, j], col=up)

    def pair(k, i, j):
        return to(piece(panel, k, j), piece(panel, k, j), pair_s.at[i, j], pair_r.at[i, j], col=mate)

    def cut(k, j):
        return panel.at[k, pl.ds(j * sub, sub), pl.ds(lane0, chip_wide)]

    def strip_first(k, i, j, side):
        return to(cut(k, j), piece(strip, k, j), sx_s.at[side, i, j], sx_r.at[i, j],
                  row=xr if side == 0 else xl)

    def strip_on(k, i, j, side):
        return to(piece(strip, k, j), piece(strip, k, j), sx_s.at[side, i, j], sx_r.at[i, j],
                  row=xr if side == 0 else xl)

    def strip_pair_first(k, i, j):
        return to(cut(k, j), piece(strip, k, j), sp_s.at[i, j], sp_r.at[i, j], col=mate)

    def strip_pair_on(k, i, j):
        return to(piece(strip, k, j), piece(strip, k, j), sp_s.at[i, j], sp_r.at[i, j], col=mate)

    def strip_local(k, i, j):
        return pltpu.make_async_copy(cut(k, j), piece(strip, k, j), loc_s.at[i, j])

    def place(d, s):
        return d * (half + 1) + s, chunk_of(d, s)

    def arrived(d, s, j):
        i, k = place(d, s)
        pair(k, i, j).start()

        @pl.when(dist == 0)
        def _():
            strip_first(k, i, j, 0).start()
            strip_first(k, i, j, 1).start()
            strip_pair_first(k, i, j).start()
            strip_local(k, i, j).start()

    def strip_step(d, s, j):
        i, k = place(d, s)

        @pl.when(dist != 0)
        def _():
            strip_on(k, i, j, 0).wait_recv()

        if d == 0:
            @pl.when(dist == 1)
            def _():
                strip_on(k, i, j, 0).start()
        else:
            @pl.when(dist == 3)
            def _():
                strip_on(k, i, j, 1).start()

        @pl.when(dist != 0)
        def _():
            strip_pair_on(k, i, j).start()

    def ready(d, s, j):
        i, k = place(d, s)
        km = k + 1 - 2 * core
        pair(km, i, j).wait_recv()
        strip_pair_on(km, i, j).wait_recv()

        @pl.when(dist == 0)
        def _():
            strip_local(k, i, j).wait()

    def work(zi):
        w0 = 2 * zi
        rows = 2 * ch
        wcol = weights[pl.ds(w0, 2)].reshape(rows, 128)
        for t in range(height // 128):
            lanes = slice(t * 128, (t + 1) * 128)
            pf = panel[pl.ds(w0, 2), :, lanes].reshape(rows, 128).astype(F32)
            wb = (pf * wcol).astype(BF)
            wpan[pl.ds(w0, 2), :, lanes] = wb.reshape(2, ch, 128)
            chir[:, lanes] += (wb.astype(F32) * pf).reshape(rows // 8, 8, 128).sum(0)
        for t in range(chip_wide // 128):
            lanes = slice(t * 128, (t + 1) * 128)
            sf = strip[pl.ds(w0, 2), :, lanes].reshape(rows, 128).astype(F32)
            wb = (sf * wcol).astype(BF).astype(F32)
            chic[:, lanes] += (wb * sf).reshape(rows // 8, 8, 128).sum(0)
        both = strip[pl.ds(w0, 2)].reshape(rows, chip_wide)
        mine = jnp.where(core == 0, both[:, :wide].astype(F32), both[:, wide:].astype(F32)).astype(BF)
        acc[...] += mm(mine, wpan[pl.ds(w0, 2)].reshape(rows, height), ((0,), (0,)))

    own = pltpu.make_async_copy(pd, panel.at[col], own_s)
    own.start()
    acc[...] = jnp.zeros_like(acc)
    chir[...] = jnp.zeros_like(chir)
    chic[...] = jnp.zeros_like(chic)
    own.wait()
    for j in range(SUBS):
        ring(0, 1, j).start()
        ring(1, 1, j).start()
    for j in range(SUBS):
        arrived(0, 0, j)

    def subs_of(d, last):
        if not last:
            return range(SUBS)
        return range(SUBS // 2) if d == 0 else range(SUBS // 2, SUBS)

    def bring(s, last, final):
        for j in range(SUBS):
            for d in (0, 1):
                if j in subs_of(d, final):
                    ring_in(d, s, j).wait_recv()
                    if not final:
                        if j in subs_of(d, last):
                            ring(d, s + 1, j).start()
                    arrived(d, s, j)

    def relay(s, final):
        for j in range(SUBS):
            for d in (0, 1):
                if j in subs_of(d, final):
                    strip_step(d, s, j)

    def settle(s, final):
        for j in range(SUBS):
            for d in (0, 1):
                if j in subs_of(d, final):
                    ready(d, s, j)

    bring(1, False, False)
    for j in range(SUBS):
        strip_step(0, 0, j)

    def early(s, carry):
        bring(s, False, False)
        relay(s - 1, False)

        @pl.when(s == 2)
        def _():
            for j in range(SUBS):
                ready(0, 0, j)

        @pl.when(s > 2)
        def _():
            settle(s - 2, False)

        def each(d, c):
            @pl.when((s > 2) | (d == 0))
            def _():
                work(chunk_of(d, s - 2) // 2)
            return c

        lax.fori_loop(0, 2, each, 0)
        return carry

    lax.fori_loop(2, half - 1, early, 0)
    def tail(s, final):
        settle(s, final)

        def each(d, c):
            work(chunk_of(d, s) // 2)
            return c
        lax.fori_loop(0, 1 if final else 2, each, 0)

    bring(half - 1, True, False)
    relay(half - 2, False)
    tail(half - 3, False)
    bring(half, False, True)
    relay(half - 1, False)
    tail(half - 2, False)
    relay(half, True)
    tail(half - 1, False)
    tail(half, True)

    s_r = rowv[0:1]
    chi_r = jnp.sum(chir[...], axis=0, keepdims=True)
    diag_r = 1.0 - s_r * chi_r * s_r
    g_r = rowv[1:2] / diag_r
    m_r = diag_r * g_r
    rvec[0:1] = g_r
    rvec[1:2] = g_r + (m_r.astype(BF).astype(F32) - m_r)
    rvec[2:3] = s_r * g_r
    chi_t = jnp.broadcast_to(jnp.sum(chic[...], axis=0, keepdims=True), chic.shape).T
    chi_c = jnp.where(core == 0, chi_t[:wide, 0:1], chi_t[wide:, 0:1])
    s_c = colv[:, 0:1]
    diag_c = 1.0 - s_c * chi_c * s_c
    g_c = colv[:, 1:2] / diag_c
    alpha = (diag_c * g_c).astype(BF).astype(F32)
    cvec[:, 0:1] = g_c
    cvec[:, 1:2] = alpha
    cvec[:, 2:3] = s_c * g_c * alpha
    cvec[:, 3:4] = s_c * g_c * alpha * alpha
    cvec[:, 4:5] = s_c

    def js(h):
        return slice(h * hj, (h + 1) * hj)

    def same(h):
        rows = lax.broadcasted_iota(jnp.int32, (hj, height), 1) + x * height
        cols = lax.broadcasted_iota(jnp.int32, (hj, height), 0) + (col * wide + h * hj)
        return rows == cols

    def begin(h):
        ident = same(h)
        e = jnp.where(ident, 1.0, 0.0) - rowv[0:1] * acc[js(h)] * cvec[js(h), 4:5]
        eps_out[js(h)] = e
        m = (e * cvec[js(h), 0:1]).astype(BF)
        mixb[js(h)] = m
        rest = m.astype(F32) - jnp.where(ident, cvec[js(h), 1:2], 0.0)
        sbuf[js(h)] = (rest * rvec[2:3]).astype(BF)

    def product(h):
        return (rvec[1:2] * mixb[js(h)].astype(F32)) - rowv[0:1] * ybuf[js(h)]

    def middle(h):
        sq = product(h) - (rowv[0:1] * acc[js(h)]) * cvec[js(h), 2:3]
        square[js(h)] = sq
        m = sq.astype(BF)
        mixb[js(h)] = m
        a = cvec[js(h), 1:2]
        rest = m.astype(F32) - jnp.where(same(h), a * a, 0.0)
        sbuf[js(h)] = (rest * rvec[2:3]).astype(BF)

    def finish(h):
        cube = product(h) - (rowv[0:1] * acc[js(h)]) * cvec[js(h), 3:4]
        mixed = eps_out[js(h)] * cvec[js(h), 0:1]
        four = jnp.where(same(h), 4.0, 0.0)
        inv_out[js(h)] = rvec[0:1] * (four - 6.0 * mixed + 4.0 * square[js(h)] - cube)

    def q_part(h, q, d):
        rows = panel[pl.ds((2 * q + d) * cpp, cpp)].reshape(pp, height)
        return mm(sbuf[js(h)], rows, ((1,), (1,)))

    def hop(u, i, src, dst, right):
        return to(src, dst, x_s.at[u, i], x_r.at[u, i], row=xr if right else xl)

    def slot(u, i, right):
        return hop(u, i, qsend.at[u, i], qrecv.at[u, i], right)

    def quarter(u, q, d):
        return qfull.at[u, q, :, pl.ds(d * pp, pp)]

    def gathered(u, i, q, d, right):
        return hop(u, i, quarter(u, q, d), quarter(u, q, d), right)

    def stage1(u, h):
        for i, q, d, right in ((0, x2, 0, False), (1, x2, 1, True), (2, xl, 1, False), (3, xr, 0, True)):
            qsend[u, i] = q_part(h, q, d).astype(BF)
            slot(u, i, right).start()
        for i, q, d in ((0, xl, 0), (1, xr, 1), (2, x, 0), (3, x, 1)):
            keep[h, i] = q_part(h, q, d)

    def stage2(u, h):
        for i, right in ((0, False), (1, True)):
            slot(u, i, right).wait_recv()
            qsend[u, 4 + i] = (keep[h, i] + qrecv[u, i].astype(F32)).astype(BF)
            slot(u, 4 + i, right).start()

    def stage3(u, h):
        for i in (2, 3):
            slot(u, i, True).wait_recv()
        for d in (0, 1):
            slot(u, 4 + d, True).wait_recv()
            direct = qrecv[u, 3 - d].astype(F32)
            total = keep[h, 2 + d] + direct + qrecv[u, 4 + d].astype(F32)
            qfull[u, x, :, d * pp:(d + 1) * pp] = total.astype(BF)
            gathered(u, 6 + d, x, d, True).start()
            gathered(u, 8 + d, x, d, False).start()

    def add(u, h, q, first):
        term = mm(qfull[u, q], wpan[pl.ds(2 * q * cpp, 2 * cpp)].reshape(2 * pp, height), ((1,), (0,)))
        if first:
            ybuf[js(h)] = term
        else:
            ybuf[js(h)] += term

    def stage4(u, h):
        add(u, h, x, True)
        gathered(u, 6, xl, 0, True).wait_recv()
        gathered(u, 10, xl, 0, True).start()
        gathered(u, 9, xr, 1, False).wait_recv()
        gathered(u, 11, xr, 1, False).start()
        gathered(u, 7, xl, 1, True).wait_recv()
        add(u, h, xl, False)
        gathered(u, 8, xr, 0, False).wait_recv()
        add(u, h, xr, False)

    def stage5(u, h):
        gathered(u, 10, x2, 0, True).wait_recv()
        gathered(u, 11, x2, 1, False).wait_recv()
        add(u, h, x2, False)

    for h in (0, 1):
        begin(h)
        stage1(h, h)
    for stage in (stage2, stage3, stage4):
        for h in (0, 1):
            stage(h, h)
    for h in (0, 1):
        stage5(h, h)
        middle(h)
        stage1(2 + h, h)
    for stage in (stage2, stage3, stage4):
        for h in (0, 1):
            stage(2 + h, h)
    for h in (0, 1):
        stage5(2 + h, h)
        finish(h)

    for u in range(4):
        for i in range(6):
            slot(u, i, True).wait_send()
        for i in range(6, 12):
            gathered(u, i, x, 0, True).wait_send()

    def drain(d, s, j):
        i, k = place(d, s)
        pair(k, i, j).wait_send()
        strip_pair_on(k, i, j).wait_send()

        @pl.when((dist == 0) | (dist == (1 if d == 0 else 3)))
        def _():
            strip_on(k, i, j, d).wait_send()

        @pl.when(dist == 0)
        def _():
            strip_on(k, i, j, 1 - d).wait_send()

    for j in range(SUBS):
        drain(0, 0, j)

        def each(s, carry):
            for d in (0, 1):
                ring(d, s, j).wait_send()
                drain(d, s, j)
            return carry

        lax.fori_loop(1, half, each, 0)
        for d in (0, 1):
            if j in subs_of(d, True):
                ring(d, half, j).wait_send()
                drain(d, half, j)


def on_device(ncol, nrow, pair_density, band_pairs, valence, conduction, wave_vectors, momentum, guess_scale):
    column_index = lax.axis_index("col")
    row_index = lax.axis_index("row")
    ch, height = pair_density.shape
    pairs = ch * ncol
    wide = height * nrow // ncol
    weight = 4.0 / (lookup(band_pairs[0], valence) - lookup(band_pairs[1], conduction))
    weights = jnp.broadcast_to(weight[:, None], (pairs, 128)).reshape(ncol, ch, 128)
    shifted = wave_vectors.astype(F32) + momentum[:, None]
    sqrt_all = jnp.sqrt(4.0 * math.pi / jnp.sum(shifted * shifted, axis=0))
    both = jnp.stack([sqrt_all, guess_scale])
    rowv = jnp.pad(lax.dynamic_slice_in_dim(both, row_index * height, height, 1), ((0, 6), (0, 0)))
    colv = jnp.pad(lax.dynamic_slice_in_dim(both, column_index * wide, wide, 1).T, ((0, 0), (0, 126)))
    half = ncol // 4
    places = 2 * (half + 1)
    hj = wide // 2
    pp = pairs // 8
    vm = pl.BlockSpec(memory_space=pltpu.VMEM)
    dma = pltpu.SemaphoreType.DMA
    out = jax.ShapeDtypeStruct((wide, height), F32)
    eps_t, inv_t = pl.pallas_call(
        functools.partial(kernel, ncol, nrow),
        out_shape=(out, out),
        in_specs=[vm] * 4,
        out_specs=(vm, vm),
        scratch_shapes=[
            pltpu.VMEM((ncol, ch, height), BF),
            pltpu.VMEM((ncol, ch, height), BF),
            pltpu.VMEM((ncol, ch, 2 * wide), BF),
            pltpu.VMEM((wide, height), F32),
            pltpu.VMEM((8, height), F32),
            pltpu.VMEM((8, 2 * wide), F32),
            pltpu.VMEM((8, height), F32),
            pltpu.VMEM((wide, 128), F32),
            pltpu.VMEM((wide, height), BF),
            pltpu.VMEM((wide, height), BF),
            pltpu.VMEM((wide, height), F32),
            pltpu.VMEM((wide, height), F32),
            pltpu.VMEM((2, 4, hj, pp), F32),
            pltpu.VMEM((4, 6, hj, pp), BF),
            pltpu.VMEM((4, 6, hj, pp), BF),
            pltpu.VMEM((4, nrow, hj, 2 * pp), BF),
            dma((2, half, SUBS)),
            dma((2, half, SUBS)),
            dma((places, SUBS)),
            dma((places, SUBS)),
            dma((2, places, SUBS)),
            dma((places, SUBS)),
            dma((places, SUBS)),
            dma((places, SUBS)),
            dma(()),
            dma((places, SUBS)),
            dma((4, 12)),
            dma((4, 12)),
        ],
        compiler_params=pltpu.CompilerParams(
            collective_id=0, has_side_effects=True, vmem_limit_bytes=60 * 1024 * 1024
        ),
        name="cohsex",
    )(pair_density, weights, rowv, colv)
    return eps_t.T, inv_t.T


def solution(mesh):
    placed = (P(("pb", "col"), "row"), P(), P(), P(), P(None, "pb"), P("pb"), P("pb"))
    return jax.shard_map(
        functools.partial(on_device, mesh.shape["col"], mesh.shape["row"]),
        mesh=mesh,
        in_specs=placed,
        out_specs=(P(("pb", "row"), "col"), P(("pb", "row"), "col")),
        check_vma=False,
    )
```

```python
import functools
import math

import jax
import jax.numpy as jnp
from jax import lax
from jax.experimental import pallas as pl
from jax.experimental.pallas import tpu as pltpu
from jax.sharding import PartitionSpec as P

MESH = pl.DeviceIdType.MESH
BF = jnp.bfloat16
F32 = jnp.float32
SUBS = 2


def mm(a, b, dims):
    return lax.dot_general(a, b, (dims, ((), ())), preferred_element_type=F32)


def kernel(ncol, nrow, pd, bands, wave, scale, valence, conduction, momentum,
           eps_out, inv_out,
           panel, wpan, strip, weights, acc, chir, chic, rvec, cvec, sbuf, mixb, square, ybuf,
           keep, qsend, qrecv, qfull,
           ring_s, ring_r, pair_s, pair_r, sx_s, sx_r, sp_s, sp_r, own_s, loc_s, x_s, x_r,
           hello, cross, known):
    nz = ncol // 2
    half = nz // 2
    per = nz // nrow
    ch, height = pd.shape
    sub = ch // SUBS
    chip_wide = strip.shape[3]
    wide = chip_wide // 2
    hj = wide // 2
    pp = keep.shape[3]
    czp = pp // ch // 2
    meet, share = half // 2 - 1, half - 2
    col = lax.axis_index("col")
    x = lax.axis_index("row")
    z = col // 2
    core = lax.rem(col, 2)
    other = 1 - core
    xr, xl = lax.rem(x + 1, nrow), lax.rem(x + nrow - 1, nrow)
    x2 = lax.rem(x + 2, nrow)
    up, down = lax.rem(col + 2, ncol), lax.rem(col + ncol - 2, ncol)
    mate = col + 1 - 2 * core
    home = z // per
    dist = lax.rem(x - home + nrow, nrow)
    lane0 = pl.multiple_of(lax.rem(z, per) * chip_wide, 128)
    odd = lax.rem(z + x, 2)
    near = (dict(col=up), dict(col=down), dict(row=xr), dict(row=xl))

    def to(src, dst, ssem, rsem, **where):
        return pltpu.make_async_remote_copy(
            src_ref=src, dst_ref=dst, send_sem=ssem, recv_sem=rsem,
            device_id=where, device_id_type=MESH)

    def tell(sem, where):
        pl.semaphore_signal(sem, inc=1, device_id=where, device_id_type=MESH)

    barrier = pltpu.get_barrier_semaphore()

    @pl.when(odd == 1)
    def _():
        for where in near:
            tell(barrier, where)
        tell(barrier, dict(col=mate))

    @pl.when(odd == 0)
    def _():
        pl.semaphore_wait(barrier, 4)
        for where in near:
            tell(hello, where)

    @pl.when(odd == 1)
    def _():
        pl.semaphore_wait(hello, 4)

    def mate_first():
        @pl.when(odd == 1)
        def _():
            pl.semaphore_wait(barrier, 1)
            tell(cross, dict(col=mate))

    def mate_second():
        @pl.when(odd == 1)
        def _():
            pl.semaphore_wait(cross, 1)
            tell(known, dict(col=down))

        @pl.when(odd == 0)
        def _():
            pl.semaphore_wait(known, 1)

    def z_of(d, s):
        return lax.rem(z + jnp.where(d == 0, nz - s, s), nz)

    def piece(ref, k, j):
        return ref.at[k, core, pl.ds(j * sub, sub)]

    def ring(d, s, j):
        src = piece(panel, z_of(d, s - 1), j)
        return to(src, src, ring_s.at[d, s - 1, j], ring_r.at[d, s - 1, j],
                  col=up if d == 0 else down)

    def ring_in(d, s, j):
        dst = piece(panel, z_of(d, s), j)
        return to(dst, dst, ring_s.at[d, s - 1, j], ring_r.at[d, s - 1, j], col=up)

    def pair(k, c, i):
        return to(panel.at[k, c], panel.at[k, c], pair_s.at[i], pair_r.at[i], col=mate)

    def strip_pair(k, c, i):
        return to(strip.at[k, c], strip.at[k, c], sp_s.at[i], sp_r.at[i], col=mate)

    def cut(k, j):
        return panel.at[k, core, pl.ds(j * sub, sub), pl.ds(lane0, chip_wide)]

    def strip_hop(k, i, j, side, first):
        return to(cut(k, j) if first else piece(strip, k, j), piece(strip, k, j),
                  sx_s.at[side, i, j], sx_r.at[i, j], row=xr if side == 0 else xl)

    def strip_local(k, i, j):
        return pltpu.make_async_copy(cut(k, j), piece(strip, k, j), loc_s.at[i, j])

    def place(d, s):
        return d * (half + 1) + s, z_of(d, s)

    def arrived(d, s, j):
        i, k = place(d, s)

        @pl.when(dist == 0)
        def _():
            strip_hop(k, i, j, 0, True).start()
            strip_hop(k, i, j, 1, True).start()
            strip_local(k, i, j).start()

    def strip_step(d, s, j):
        i, k = place(d, s)

        @pl.when(dist == 0)
        def _():
            strip_local(k, i, j).wait()

        @pl.when(dist != 0)
        def _():
            strip_hop(k, i, j, 0, False).wait_recv()

        @pl.when(dist == (1 if d == 0 else 3))
        def _():
            strip_hop(k, i, j, d, False).start()

    def give(d, s):
        i, k = place(d, s)
        pair(k, core, i).start()
        strip_pair(k, core, i).start()

    def take(d, s):
        i, k = place(d, s)
        pair(k, other, i).wait_recv()
        strip_pair(k, other, i).wait_recv()

    def work(za, zb, c):
        def one(n, carry):
            k = jnp.where(n == 0, za, zb)
            wcol = weights[pl.ds(pl.multiple_of((2 * k + c) * ch, 8), ch)]
            for t in range(height // 128):
                lanes = slice(t * 128, (t + 1) * 128)
                pf = panel[k, c, :, lanes].astype(F32)
                wb = (pf * wcol).astype(BF)
                wpan[k, c, :, lanes] = wb
                chir[:, lanes] += (wb.astype(F32) * pf).reshape(ch // 8, 8, 128).sum(0)
            for t in range(chip_wide // 128):
                lanes = slice(t * 128, (t + 1) * 128)
                sf = strip[k, c, :, lanes].astype(F32)
                wb = (sf * wcol).astype(BF).astype(F32)
                chic[:, lanes] += (wb * sf).reshape(ch // 8, 8, 128).sum(0)
            return carry

        lax.fori_loop(0, 2, one, 0)
        both = jnp.concatenate([strip[za, c], strip[zb, c]], axis=0)
        mine = jnp.where(core == 0, both[:, :wide].astype(F32), both[:, wide:].astype(F32)).astype(BF)
        acc[...] += mm(mine, jnp.concatenate([wpan[za, c], wpan[zb, c]], axis=0), ((0,), (0,)))

    own = pltpu.make_async_copy(pd, panel.at[z, core], own_s)
    own.start()
    own.wait()
    for j in range(SUBS):
        ring(0, 1, j).start()
        ring(1, 1, j).start()
    for j in range(SUBS):
        arrived(0, 0, j)
    acc[...] = jnp.zeros_like(acc)
    chir[...] = jnp.zeros_like(chir)
    chic[...] = jnp.zeros_like(chic)

    def look(ids, table):
        def level(v, found):
            return jnp.where(ids == v, table[v], found)
        return lax.fori_loop(0, table.shape[0], level, jnp.zeros(ids.shape, F32), unroll=4)

    weight = 4.0 / (look(bands[0:1], valence) - look(bands[1:2], conduction))
    for t in range(weights.shape[0] // 128):
        lanes = slice(t * 128, (t + 1) * 128)
        weights[lanes] = jnp.broadcast_to(weight[:, lanes], (128, 128)).T

    def subs_of(d, last):
        if not last:
            return range(SUBS)
        return range(SUBS // 2) if d == 0 else range(SUBS // 2, SUBS)

    def bring(s, last, final):
        for j in range(SUBS):
            for d in (0, 1):
                if j in subs_of(d, final):
                    ring_in(d, s, j).wait_recv()
                    if not final and j in subs_of(d, last):
                        ring(d, s + 1, j).start()
                    arrived(d, s, j)

    def relay(s, final):
        for j in range(SUBS):
            for d in (0, 1):
                if j in subs_of(d, final):
                    strip_step(d, s, j)

    def unit(s, c):
        work(z_of(0, s), z_of(1, s), c)

    bring(1, False, False)
    for j in range(SUBS):
        strip_step(0, 0, j)

    def step(s, carry):
        bring(s, False, False)
        relay(s - 1, False)

        @pl.when(s == meet)
        def _():
            mate_first()

        @pl.when(s == share)
        def _():
            mate_second()
            give(0, 0)

            def bulk(r, c):
                give(0, r)
                give(1, r)
                return c
            lax.fori_loop(1, share, bulk, 0)

        unit(s - 1, core)
        return carry

    if meet < 2:
        mate_first()
    lax.fori_loop(2, half - 1, step, 0)
    bring(half - 1, True, False)
    relay(half - 2, False)
    give(0, half - 2)
    give(1, half - 2)
    unit(half - 2, core)
    bring(half, False, True)
    relay(half - 1, False)
    give(0, half - 1)
    give(1, half - 1)
    unit(half - 1, core)
    relay(half, True)
    give(0, half)
    work(z, z_of(0, half), core)

    def mates(s, carry):
        take(0, s)
        take(1, s)
        unit(s, other)
        return carry

    lax.fori_loop(1, half, mates, 0)
    take(0, 0)
    take(0, half)
    work(z, z_of(0, half), other)

    def root(first, count):
        lanes = pl.ds(pl.multiple_of(first, 128), count)
        total = jnp.zeros((1, count), F32)
        for i in range(3):
            shifted = wave[i:i + 1, lanes].astype(F32) + momentum[i]
            total = total + shifted * shifted
        return jnp.sqrt(4.0 * math.pi / total), scale[:, lanes]

    s_r, t_r = root(x * height, height)
    chi_r = jnp.sum(chir[...], axis=0, keepdims=True)
    diag_r = 1.0 - s_r * chi_r * s_r
    g_r = t_r / diag_r
    m_r = diag_r * g_r
    rvec[0:1] = g_r
    rvec[1:2] = g_r + (m_r.astype(BF).astype(F32) - m_r)
    rvec[2:3] = s_r * g_r
    rvec[3:4] = s_r
    s_l, t_l = root(z * chip_wide, chip_wide)
    chi_l = jnp.sum(chic[...], axis=0, keepdims=True)
    chic[0:1] = s_l
    chic[1:2] = t_l
    chic[2:3] = chi_l
    turned = chic[...].T
    turned = jnp.where(core == 0, turned[:wide], turned[wide:])
    s_c = turned[:, 0:1]
    diag_c = 1.0 - s_c * turned[:, 2:3] * s_c
    g_c = turned[:, 1:2] / diag_c
    alpha = (diag_c * g_c).astype(BF).astype(F32)
    cvec[:, 0:1] = g_c
    cvec[:, 1:2] = alpha
    cvec[:, 2:3] = s_c * g_c * alpha
    cvec[:, 3:4] = s_c * g_c * alpha * alpha
    cvec[:, 4:5] = s_c

    def js(h):
        return slice(h * hj, (h + 1) * hj)

    def same(h):
        rows = lax.broadcasted_iota(jnp.int32, (hj, height), 1) + x * height
        cols = lax.broadcasted_iota(jnp.int32, (hj, height), 0) + (col * wide + h * hj)
        return rows == cols

    def begin(h):
        ident = same(h)
        e = jnp.where(ident, 1.0, 0.0) - rvec[3:4] * acc[js(h)] * cvec[js(h), 4:5]
        eps_out[js(h)] = e
        m = (e * cvec[js(h), 0:1]).astype(BF)
        mixb[js(h)] = m
        rest = m.astype(F32) - jnp.where(ident, cvec[js(h), 1:2], 0.0)
        sbuf[js(h)] = (rest * rvec[2:3]).astype(BF)

    def product(h):
        return (rvec[1:2] * mixb[js(h)].astype(F32)) - rvec[3:4] * ybuf[js(h)]

    def middle(h):
        sq = product(h) - (rvec[3:4] * acc[js(h)]) * cvec[js(h), 2:3]
        square[js(h)] = sq
        m = sq.astype(BF)
        mixb[js(h)] = m
        a = cvec[js(h), 1:2]
        rest = m.astype(F32) - jnp.where(same(h), a * a, 0.0)
        sbuf[js(h)] = (rest * rvec[2:3]).astype(BF)

    def finish(h):
        cube = product(h) - (rvec[3:4] * acc[js(h)]) * cvec[js(h), 3:4]
        mixed = eps_out[js(h)] * cvec[js(h), 0:1]
        four = jnp.where(same(h), 4.0, 0.0)
        inv_out[js(h)] = rvec[0:1] * (four - 6.0 * mixed + 4.0 * square[js(h)] - cube)

    def q_part(h, q, d):
        rows = panel[pl.ds((2 * q + d) * czp, czp)].reshape(pp, height)
        return mm(sbuf[js(h)], rows, ((1,), (1,)))

    def hop(u, i, src, dst, right):
        return to(src, dst, x_s.at[u, i], x_r.at[u, i], row=xr if right else xl)

    def slot(u, i, right):
        return hop(u, i, qsend.at[u, i], qrecv.at[u, i], right)

    def quarter(u, q, d):
        return qfull.at[u, q, :, pl.ds(d * pp, pp)]

    def gathered(u, i, q, d, right):
        return hop(u, i, quarter(u, q, d), quarter(u, q, d), right)

    def stage1(u, h):
        for i, q, d, right in ((0, x2, 0, False), (1, x2, 1, True), (2, xl, 1, False), (3, xr, 0, True)):
            qsend[u, i] = q_part(h, q, d).astype(BF)
            slot(u, i, right).start()
        for i, q, d in ((0, xl, 0), (1, xr, 1), (2, x, 0), (3, x, 1)):
            keep[h, i] = q_part(h, q, d)

    def stage2(u, h):
        for i, right in ((0, False), (1, True)):
            slot(u, i, right).wait_recv()
            qsend[u, 4 + i] = (keep[h, i] + qrecv[u, i].astype(F32)).astype(BF)
            slot(u, 4 + i, right).start()

    def stage3(u, h):
        for i in (2, 3):
            slot(u, i, True).wait_recv()
        for d in (0, 1):
            slot(u, 4 + d, True).wait_recv()
            direct = qrecv[u, 3 - d].astype(F32)
            total = keep[h, 2 + d] + direct + qrecv[u, 4 + d].astype(F32)
            qfull[u, x, :, d * pp:(d + 1) * pp] = total.astype(BF)
            gathered(u, 6 + d, x, d, True).start()
            gathered(u, 8 + d, x, d, False).start()

    def add(u, h, q, first):
        term = mm(qfull[u, q], wpan[pl.ds(2 * q * czp, 2 * czp)].reshape(2 * pp, height), ((1,), (0,)))
        if first:
            ybuf[js(h)] = term
        else:
            ybuf[js(h)] += term

    def stage4(u, h):
        add(u, h, x, True)
        gathered(u, 6, xl, 0, True).wait_recv()
        gathered(u, 10, xl, 0, True).start()
        gathered(u, 9, xr, 1, False).wait_recv()
        gathered(u, 11, xr, 1, False).start()
        gathered(u, 7, xl, 1, True).wait_recv()
        add(u, h, xl, False)
        gathered(u, 8, xr, 0, False).wait_recv()
        add(u, h, xr, False)

    def stage5(u, h):
        gathered(u, 10, x2, 0, True).wait_recv()
        gathered(u, 11, x2, 1, False).wait_recv()
        add(u, h, x2, False)

    for h in (0, 1):
        begin(h)
        stage1(h, h)
    for stage in (stage2, stage3, stage4):
        for h in (0, 1):
            stage(h, h)
    for h in (0, 1):
        stage5(h, h)
        middle(h)
        stage1(2 + h, h)
    for stage in (stage2, stage3, stage4):
        for h in (0, 1):
            stage(2 + h, h)
    for h in (0, 1):
        stage5(2 + h, h)
        finish(h)

    for u in range(4):
        for i in range(6):
            slot(u, i, True).wait_send()
        for i in range(6, 12):
            gathered(u, i, x, 0, True).wait_send()

    def drain(d, s, subs):
        i, k = place(d, s)
        for j in subs:
            @pl.when((dist == 0) | (dist == (1 if d == 0 else 3)))
            def _():
                strip_hop(k, i, j, d, False).wait_send()

            @pl.when(dist == 0)
            def _():
                strip_hop(k, i, j, 1 - d, False).wait_send()

    def given(d, s):
        i, k = place(d, s)
        pair(k, core, i).wait_send()
        strip_pair(k, core, i).wait_send()

    def each(s, carry):
        for d in (0, 1):
            for j in range(SUBS):
                ring(d, s, j).wait_send()
            drain(d, s, range(SUBS))
            given(d, s)
        return carry

    drain(0, 0, range(SUBS))
    given(0, 0)
    lax.fori_loop(1, half, each, 0)
    for d in (0, 1):
        for j in subs_of(d, True):
            ring(d, half, j).wait_send()
        drain(d, half, subs_of(d, True))
    given(0, half)


def on_device(ncol, nrow, pair_density, band_pairs, valence, conduction, wave_vectors, momentum, guess_scale):
    ch, height = pair_density.shape
    pairs = ch * ncol
    nz = ncol // 2
    wide = height * nrow // ncol
    half = nz // 2
    places = 2 * (half + 1)
    hj = wide // 2
    pp = pairs // 8
    vm = pl.BlockSpec(memory_space=pltpu.VMEM)
    sm = pl.BlockSpec(memory_space=pltpu.SMEM)
    dma = pltpu.SemaphoreType.DMA
    out = jax.ShapeDtypeStruct((wide, height), F32)
    eps_t, inv_t = pl.pallas_call(
        functools.partial(kernel, ncol, nrow),
        out_shape=(out, out),
        in_specs=[pl.BlockSpec(memory_space=pl.ANY), vm, vm, vm, sm, sm, sm],
        out_specs=(vm, vm),
        scratch_shapes=[
            pltpu.VMEM((nz, 2, ch, height), BF),
            pltpu.VMEM((nz, 2, ch, height), BF),
            pltpu.VMEM((nz, 2, ch, 2 * wide), BF),
            pltpu.VMEM((pairs, 128), F32),
            pltpu.VMEM((wide, height), F32),
            pltpu.VMEM((8, height), F32),
            pltpu.VMEM((8, 2 * wide), F32),
            pltpu.VMEM((8, height), F32),
            pltpu.VMEM((wide, 128), F32),
            pltpu.VMEM((wide, height), BF),
            pltpu.VMEM((wide, height), BF),
            pltpu.VMEM((wide, height), F32),
            pltpu.VMEM((wide, height), F32),
            pltpu.VMEM((2, 4, hj, pp), F32),
            pltpu.VMEM((4, 6, hj, pp), BF),
            pltpu.VMEM((4, 6, hj, pp), BF),
            pltpu.VMEM((4, nrow, hj, 2 * pp), BF),
            dma((2, half, SUBS)),
            dma((2, half, SUBS)),
            dma((places,)),
            dma((places,)),
            dma((2, places, SUBS)),
            dma((places, SUBS)),
            dma((places,)),
            dma((places,)),
            dma(()),
            dma((places, SUBS)),
            dma((4, 12)),
            dma((4, 12)),
            pltpu.SemaphoreType.REGULAR,
            pltpu.SemaphoreType.REGULAR,
            pltpu.SemaphoreType.REGULAR,
        ],
        compiler_params=pltpu.CompilerParams(
            collective_id=0, has_side_effects=True, vmem_limit_bytes=44 * 1024 * 1024
        ),
        name="cohsex",
    )(pair_density, band_pairs, wave_vectors, guess_scale[None, :], valence, conduction, momentum)
    return eps_t.T, inv_t.T


def solution(mesh):
    placed = (P(("pb", "col"), "row"), P(), P(), P(), P(None, "pb"), P("pb"), P("pb"))
    return jax.shard_map(
        functools.partial(on_device, mesh.shape["col"], mesh.shape["row"]),
        mesh=mesh,
        in_specs=placed,
        out_specs=(P(("pb", "row"), "col"), P(("pb", "row"), "col")),
        check_vma=False,
    )
```

```python
import functools
import math

import jax
import jax.numpy as jnp
from jax import lax
from jax.experimental import pallas as pl
from jax.experimental.pallas import tpu as pltpu
from jax.sharding import PartitionSpec as P

MESH = pl.DeviceIdType.MESH
BF = jnp.bfloat16
F32 = jnp.float32
SUBS = 2


def mm(a, b, dims):
    return lax.dot_general(a, b, (dims, ((), ())), preferred_element_type=F32)


def kernel(ncol, nrow, pd, bands_in, wave_in, scale_in, valence, conduction, momentum,
           eps_out, inv_out,
           bands, wave, scale, weights, panel, wpan, strip, acc, chir, chic, rvec, cvec, sbuf, mixb, square, ybuf,
           keep, qsend, qrecv, qfull,
           in_s, ring_s, ring_r, pair_s, pair_r, sx_s, sx_r, sp_s, sp_r, own_s, loc_s, x_s, x_r):
    nz = ncol // 2
    half = nz // 2
    per = nz // nrow
    ch, height = pd.shape
    sub = ch // SUBS
    chip_wide = strip.shape[2]
    wide = chip_wide // 2
    hj = wide // 2
    pp = keep.shape[3]
    cpp = pp // ch
    col = lax.axis_index("col")
    x = lax.axis_index("row")
    z = col // 2
    core = lax.rem(col, 2)
    xr, xl = lax.rem(x + 1, nrow), lax.rem(x + nrow - 1, nrow)
    x2 = lax.rem(x + 2, nrow)
    up, down = lax.rem(col + 2, ncol), lax.rem(col + ncol - 2, ncol)
    mate = col + 1 - 2 * core
    home = z // per
    dist = lax.rem(x - home + nrow, nrow)
    lane0 = pl.multiple_of(lax.rem(z, per) * chip_wide, 128)

    def to(src, dst, ssem, rsem, **where):
        return pltpu.make_async_remote_copy(
            src_ref=src, dst_ref=dst, send_sem=ssem, recv_sem=rsem,
            device_id=where, device_id_type=MESH)

    own = pltpu.make_async_copy(pd, panel.at[col], own_s)
    own.start()
    small = [pltpu.make_async_copy(a, b, in_s.at[i])
             for i, (a, b) in enumerate(((bands_in, bands), (wave_in, wave), (scale_in, scale)))]
    for copy in small:
        copy.start()
    barrier = pltpu.get_barrier_semaphore()
    for where in (dict(col=up), dict(col=down), dict(col=mate), dict(row=xr), dict(row=xl)):
        pl.semaphore_signal(barrier, inc=1, device_id=where, device_id_type=MESH)
    pl.semaphore_wait(barrier, 5)

    def chunk_of(d, s):
        away = jnp.where(d == 0, nz - s, s)
        return 2 * lax.rem(z + away, nz) + core

    def piece(ref, k, j):
        return ref.at[k, pl.ds(j * sub, sub)]

    def ring(d, s, j):
        k = chunk_of(d, s - 1)
        src = piece(panel, k, j)
        return to(src, piece(panel, k, j), ring_s.at[d, s - 1, j], ring_r.at[d, s - 1, j],
                  col=up if d == 0 else down)

    def ring_in(d, s, j):
        k = chunk_of(d, s)
        return to(piece(panel, k, j), piece(panel, k, j), ring_s.at[d, s - 1, j],
                  ring_r.at[d, s - 1, j], col=up)

    def pair(k, i, j):
        return to(piece(panel, k, j), piece(panel, k, j), pair_s.at[i, j], pair_r.at[i, j], col=mate)

    def cut(k, j):
        return panel.at[k, pl.ds(j * sub, sub), pl.ds(lane0, chip_wide)]

    def strip_first(k, i, j, side):
        return to(cut(k, j), piece(strip, k, j), sx_s.at[side, i, j], sx_r.at[i, j],
                  row=xr if side == 0 else xl)

    def strip_on(k, i, j, side):
        return to(piece(strip, k, j), piece(strip, k, j), sx_s.at[side, i, j], sx_r.at[i, j],
                  row=xr if side == 0 else xl)

    def strip_pair_first(k, i, j):
        return to(cut(k, j), piece(strip, k, j), sp_s.at[i, j], sp_r.at[i, j], col=mate)

    def strip_pair_on(k, i, j):
        return to(piece(strip, k, j), piece(strip, k, j), sp_s.at[i, j], sp_r.at[i, j], col=mate)

    def strip_local(k, i, j):
        return pltpu.make_async_copy(cut(k, j), piece(strip, k, j), loc_s.at[i, j])

    def place(d, s):
        return d * (half + 1) + s, chunk_of(d, s)

    def arrived(d, s, j):
        i, k = place(d, s)
        pair(k, i, j).start()

        @pl.when(dist == 0)
        def _():
            strip_first(k, i, j, 0).start()
            strip_first(k, i, j, 1).start()
            strip_pair_first(k, i, j).start()
            strip_local(k, i, j).start()

    def strip_step(d, s, j):
        i, k = place(d, s)

        @pl.when(dist != 0)
        def _():
            strip_on(k, i, j, 0).wait_recv()

        if d == 0:
            @pl.when(dist == 1)
            def _():
                strip_on(k, i, j, 0).start()
        else:
            @pl.when(dist == 3)
            def _():
                strip_on(k, i, j, 1).start()

        @pl.when(dist != 0)
        def _():
            strip_pair_on(k, i, j).start()

    def ready(d, s, j):
        i, k = place(d, s)
        km = k + 1 - 2 * core
        pair(km, i, j).wait_recv()
        strip_pair_on(km, i, j).wait_recv()

        @pl.when(dist == 0)
        def _():
            strip_local(k, i, j).wait()

    def work(zi):
        w0 = 2 * zi
        rows = 2 * ch
        wcol = weights[pl.ds(pl.multiple_of(w0 * ch, 8), rows)]
        for t in range(height // 128):
            lanes = slice(t * 128, (t + 1) * 128)
            pf = panel[pl.ds(w0, 2), :, lanes].reshape(rows, 128).astype(F32)
            wb = (pf * wcol).astype(BF)
            wpan[pl.ds(w0, 2), :, lanes] = wb.reshape(2, ch, 128)
            chir[:, lanes] += (wb.astype(F32) * pf).reshape(rows // 8, 8, 128).sum(0)
        for t in range(chip_wide // 128):
            lanes = slice(t * 128, (t + 1) * 128)
            sf = strip[pl.ds(w0, 2), :, lanes].reshape(rows, 128).astype(F32)
            wb = (sf * wcol).astype(BF).astype(F32)
            chic[:, lanes] += (wb * sf).reshape(rows // 8, 8, 128).sum(0)
        both = strip[pl.ds(w0, 2)].reshape(rows, chip_wide)
        mine = jnp.where(core == 0, both[:, :wide].astype(F32), both[:, wide:].astype(F32)).astype(BF)
        acc[...] += mm(mine, wpan[pl.ds(w0, 2)].reshape(rows, height), ((0,), (0,)))

    own.wait()
    for j in range(SUBS):
        ring(0, 1, j).start()
        ring(1, 1, j).start()
    for j in range(SUBS):
        arrived(0, 0, j)
    acc[...] = jnp.zeros_like(acc)
    chir[...] = jnp.zeros_like(chir)
    chic[...] = jnp.zeros_like(chic)
    for copy in small:
        copy.wait()

    def look(ids, table):
        def level(v, found):
            return jnp.where(ids == v, table[v], found)
        return lax.fori_loop(0, table.shape[0], level, jnp.zeros(ids.shape, F32), unroll=4)

    weight = 4.0 / (look(bands[0:1], valence) - look(bands[1:2], conduction))
    for t in range(weights.shape[0] // 128):
        lanes = slice(t * 128, (t + 1) * 128)
        weights[lanes] = jnp.broadcast_to(weight[:, lanes], (128, 128)).T

    def subs_of(d, last):
        if not last:
            return range(SUBS)
        return range(SUBS // 2) if d == 0 else range(SUBS // 2, SUBS)

    def bring(s, last, final):
        for j in range(SUBS):
            for d in (0, 1):
                if j in subs_of(d, final):
                    ring_in(d, s, j).wait_recv()
                    if not final:
                        if j in subs_of(d, last):
                            ring(d, s + 1, j).start()
                    arrived(d, s, j)

    def relay(s, final):
        for j in range(SUBS):
            for d in (0, 1):
                if j in subs_of(d, final):
                    strip_step(d, s, j)

    def settle(s, final):
        for j in range(SUBS):
            for d in (0, 1):
                if j in subs_of(d, final):
                    ready(d, s, j)

    bring(1, False, False)
    for j in range(SUBS):
        strip_step(0, 0, j)

    def early(s, carry):
        bring(s, False, False)
        relay(s - 1, False)

        @pl.when(s == 2)
        def _():
            for j in range(SUBS):
                ready(0, 0, j)

        @pl.when(s > 2)
        def _():
            settle(s - 2, False)

        def each(d, c):
            @pl.when((s > 2) | (d == 0))
            def _():
                work(chunk_of(d, s - 2) // 2)
            return c

        lax.fori_loop(0, 2, each, 0)
        return carry

    lax.fori_loop(2, half - 1, early, 0)
    def tail(s, final):
        settle(s, final)

        def each(d, c):
            work(chunk_of(d, s) // 2)
            return c
        lax.fori_loop(0, 1 if final else 2, each, 0)

    bring(half - 1, True, False)
    relay(half - 2, False)
    tail(half - 3, False)
    bring(half, False, True)
    relay(half - 1, False)
    tail(half - 2, False)
    relay(half, True)
    tail(half - 1, False)
    tail(half, True)

    def root(first, count):
        lanes = pl.ds(pl.multiple_of(first, 128), count)
        total = jnp.zeros((1, count), F32)
        for i in range(3):
            shifted = wave[i:i + 1, lanes].astype(F32) + momentum[i]
            total = total + shifted * shifted
        return jnp.sqrt(4.0 * math.pi / total), scale[:, lanes]

    s_r, t_r = root(x * height, height)
    chi_r = jnp.sum(chir[...], axis=0, keepdims=True)
    diag_r = 1.0 - s_r * chi_r * s_r
    g_r = t_r / diag_r
    m_r = diag_r * g_r
    rvec[0:1] = g_r
    rvec[1:2] = g_r + (m_r.astype(BF).astype(F32) - m_r)
    rvec[2:3] = s_r * g_r
    rvec[3:4] = s_r
    s_l, t_l = root(z * chip_wide, chip_wide)
    chi_l = jnp.sum(chic[...], axis=0, keepdims=True)
    chic[0:1] = s_l
    chic[1:2] = t_l
    chic[2:3] = chi_l
    turned = chic[...].T
    turned = jnp.where(core == 0, turned[:wide], turned[wide:])
    s_c = turned[:, 0:1]
    diag_c = 1.0 - s_c * turned[:, 2:3] * s_c
    g_c = turned[:, 1:2] / diag_c
    alpha = (diag_c * g_c).astype(BF).astype(F32)
    cvec[:, 0:1] = g_c
    cvec[:, 1:2] = alpha
    cvec[:, 2:3] = s_c * g_c * alpha
    cvec[:, 3:4] = s_c * g_c * alpha * alpha
    cvec[:, 4:5] = s_c

    def js(h):
        return slice(h * hj, (h + 1) * hj)

    def same(h):
        rows = lax.broadcasted_iota(jnp.int32, (hj, height), 1) + x * height
        cols = lax.broadcasted_iota(jnp.int32, (hj, height), 0) + (col * wide + h * hj)
        return rows == cols

    def begin(h):
        ident = same(h)
        e = jnp.where(ident, 1.0, 0.0) - rvec[3:4] * acc[js(h)] * cvec[js(h), 4:5]
        eps_out[js(h)] = e
        m = (e * cvec[js(h), 0:1]).astype(BF)
        mixb[js(h)] = m
        rest = m.astype(F32) - jnp.where(ident, cvec[js(h), 1:2], 0.0)
        sbuf[js(h)] = (rest * rvec[2:3]).astype(BF)

    def product(h):
        return (rvec[1:2] * mixb[js(h)].astype(F32)) - rvec[3:4] * ybuf[js(h)]

    def middle(h):
        sq = product(h) - (rvec[3:4] * acc[js(h)]) * cvec[js(h), 2:3]
        square[js(h)] = sq
        m = sq.astype(BF)
        mixb[js(h)] = m
        a = cvec[js(h), 1:2]
        rest = m.astype(F32) - jnp.where(same(h), a * a, 0.0)
        sbuf[js(h)] = (rest * rvec[2:3]).astype(BF)

    def finish(h):
        cube = product(h) - (rvec[3:4] * acc[js(h)]) * cvec[js(h), 3:4]
        mixed = eps_out[js(h)] * cvec[js(h), 0:1]
        four = jnp.where(same(h), 4.0, 0.0)
        inv_out[js(h)] = rvec[0:1] * (four - 6.0 * mixed + 4.0 * square[js(h)] - cube)

    def q_part(h, q, d):
        rows = panel[pl.ds((2 * q + d) * cpp, cpp)].reshape(pp, height)
        return mm(sbuf[js(h)], rows, ((1,), (1,)))

    def hop(u, i, src, dst, right):
        return to(src, dst, x_s.at[u, i], x_r.at[u, i], row=xr if right else xl)

    def slot(u, i, right):
        return hop(u, i, qsend.at[u, i], qrecv.at[u, i], right)

    def quarter(u, q, d):
        return qfull.at[u, q, :, pl.ds(d * pp, pp)]

    def gathered(u, i, q, d, right):
        return hop(u, i, quarter(u, q, d), quarter(u, q, d), right)

    def stage1(u, h):
        for i, q, d, right in ((0, x2, 0, False), (1, x2, 1, True), (2, xl, 1, False), (3, xr, 0, True)):
            qsend[u, i] = q_part(h, q, d).astype(BF)
            slot(u, i, right).start()

    def stage1_kept(h):
        for i, q, d in ((0, xl, 0), (1, xr, 1), (2, x, 0), (3, x, 1)):
            keep[h, i] = q_part(h, q, d)

    def stage2(u, h):
        for i, right in ((0, False), (1, True)):
            slot(u, i, right).wait_recv()
            qsend[u, 4 + i] = (keep[h, i] + qrecv[u, i].astype(F32)).astype(BF)
            slot(u, 4 + i, right).start()

    def stage3(u, h):
        for i in (2, 3):
            slot(u, i, True).wait_recv()
        for d in (0, 1):
            slot(u, 4 + d, True).wait_recv()
            direct = qrecv[u, 3 - d].astype(F32)
            total = keep[h, 2 + d] + direct + qrecv[u, 4 + d].astype(F32)
            qfull[u, x, :, d * pp:(d + 1) * pp] = total.astype(BF)
            gathered(u, 6 + d, x, d, True).start()
            gathered(u, 8 + d, x, d, False).start()

    def add(u, h, q, first):
        term = mm(qfull[u, q], wpan[pl.ds(2 * q * cpp, 2 * cpp)].reshape(2 * pp, height), ((1,), (0,)))
        if first:
            ybuf[js(h)] = term
        else:
            ybuf[js(h)] += term

    def stage4(u, h):
        add(u, h, x, True)
        gathered(u, 6, xl, 0, True).wait_recv()
        gathered(u, 10, xl, 0, True).start()
        gathered(u, 9, xr, 1, False).wait_recv()
        gathered(u, 11, xr, 1, False).start()
        gathered(u, 7, xl, 1, True).wait_recv()
        add(u, h, xl, False)
        gathered(u, 8, xr, 0, False).wait_recv()
        add(u, h, xr, False)

    def stage5(u, h):
        gathered(u, 10, x2, 0, True).wait_recv()
        gathered(u, 11, x2, 1, False).wait_recv()
        add(u, h, x2, False)

    for h in (0, 1):
        begin(h)
        stage1(h, h)
    for h in (0, 1):
        stage1_kept(h)
    for stage in (stage2, stage3, stage4):
        for h in (0, 1):
            stage(h, h)
    for h in (0, 1):
        stage5(h, h)
        middle(h)
        stage1(2 + h, h)
    for h in (0, 1):
        stage1_kept(h)
    for stage in (stage2, stage3, stage4):
        for h in (0, 1):
            stage(2 + h, h)
    for h in (0, 1):
        stage5(2 + h, h)
        finish(h)

    for u in range(4):
        for i in range(6):
            slot(u, i, True).wait_send()
        for i in range(6, 12):
            gathered(u, i, x, 0, True).wait_send()

    def drain(d, s, j):
        i, k = place(d, s)
        pair(k, i, j).wait_send()
        strip_pair_on(k, i, j).wait_send()

        @pl.when((dist == 0) | (dist == (1 if d == 0 else 3)))
        def _():
            strip_on(k, i, j, d).wait_send()

        @pl.when(dist == 0)
        def _():
            strip_on(k, i, j, 1 - d).wait_send()

    for j in range(SUBS):
        drain(0, 0, j)

        def each(s, carry):
            for d in (0, 1):
                ring(d, s, j).wait_send()
                drain(d, s, j)
            return carry

        lax.fori_loop(1, half, each, 0)
        for d in (0, 1):
            if j in subs_of(d, True):
                ring(d, half, j).wait_send()
                drain(d, half, j)


def on_device(ncol, nrow, pair_density, band_pairs, valence, conduction, wave_vectors, momentum, guess_scale):
    ch, height = pair_density.shape
    pairs = ch * ncol
    wide = height * nrow // ncol
    scales = guess_scale[None, :]
    half = ncol // 4
    places = 2 * (half + 1)
    hj = wide // 2
    pp = pairs // 8
    vm = pl.BlockSpec(memory_space=pltpu.VMEM)
    sm = pl.BlockSpec(memory_space=pltpu.SMEM)
    hbm = pl.BlockSpec(memory_space=pltpu.HBM)
    dma = pltpu.SemaphoreType.DMA
    out = jax.ShapeDtypeStruct((wide, height), F32)
    eps_t, inv_t = pl.pallas_call(
        functools.partial(kernel, ncol, nrow),
        out_shape=(pltpu.VMEM((wide, height), F32), pltpu.VMEM((wide, height), F32)),
        in_specs=[hbm, hbm, hbm, hbm, sm, sm, sm],
        out_specs=(vm, vm),
        scratch_shapes=[
            pltpu.VMEM(band_pairs.shape, jnp.int32),
            pltpu.VMEM(wave_vectors.shape, jnp.int32),
            pltpu.VMEM(scales.shape, F32),
            pltpu.VMEM((pairs, 128), F32),
            pltpu.VMEM((ncol, ch, height), BF),
            pltpu.VMEM((ncol, ch, height), BF),
            pltpu.VMEM((ncol, ch, 2 * wide), BF),
            pltpu.VMEM((wide, height), F32),
            pltpu.VMEM((8, height), F32),
            pltpu.VMEM((8, 2 * wide), F32),
            pltpu.VMEM((8, height), F32),
            pltpu.VMEM((wide, 128), F32),
            pltpu.VMEM((wide, height), BF),
            pltpu.VMEM((wide, height), BF),
            pltpu.VMEM((wide, height), F32),
            pltpu.VMEM((wide, height), F32),
            pltpu.VMEM((2, 4, hj, pp), F32),
            pltpu.VMEM((4, 6, hj, pp), BF),
            pltpu.VMEM((4, 6, hj, pp), BF),
            pltpu.VMEM((4, nrow, hj, 2 * pp), BF),
            dma((3,)),
            dma((2, half, SUBS)),
            dma((2, half, SUBS)),
            dma((places, SUBS)),
            dma((places, SUBS)),
            dma((2, places, SUBS)),
            dma((places, SUBS)),
            dma((places, SUBS)),
            dma((places, SUBS)),
            dma(()),
            dma((places, SUBS)),
            dma((4, 12)),
            dma((4, 12)),
        ],
        compiler_params=pltpu.CompilerParams(
            collective_id=0, has_side_effects=True, vmem_limit_bytes=60 * 1024 * 1024
        ),
        name="cohsex",
    )(pair_density, band_pairs, wave_vectors, scales, valence, conduction, momentum)
    return eps_t.T, inv_t.T


def solution(mesh):
    placed = (P(("pb", "col"), "row"), P(), P(), P(), P(None, "pb"), P("pb"), P("pb"))
    return jax.shard_map(
        functools.partial(on_device, mesh.shape["col"], mesh.shape["row"]),
        mesh=mesh,
        in_specs=placed,
        out_specs=(P(("pb", "row"), "col"), P(("pb", "row"), "col")),
        check_vma=False,
    )
```

```python
import functools
import math

import jax
import jax.numpy as jnp
from jax import lax
from jax.experimental import pallas as pl
from jax.experimental.pallas import tpu as pltpu
from jax.sharding import PartitionSpec as P

MESH = pl.DeviceIdType.MESH
BF = jnp.bfloat16
F32 = jnp.float32
SUBS = 2


def mm(a, b, dims):
    return lax.dot_general(a, b, (dims, ((), ())), preferred_element_type=F32)


def kernel(ncol, nrow, pd, bands_in, wave_in, scale_in, valence_in, conduction_in, momentum_in,
           eps_out, inv_out,
           bands, wave, scale, valence, conduction, momentum, weights, panel, wpan, strip, acc, chir, chic, rvec, cvec, sbuf, mixb, square, ybuf,
           keep, qsend, qrecv, qfull,
           in_s, ring_s, ring_r, pair_s, pair_r, sx_s, sx_r, sp_s, sp_r, own_s, loc_s, x_s, x_r):
    nz = ncol // 2
    half = nz // 2
    per = nz // nrow
    ch, height = pd.shape
    sub = ch // SUBS
    chip_wide = strip.shape[2]
    wide = chip_wide // 2
    hj = wide // 2
    pp = keep.shape[3]
    cpp = pp // ch
    col = lax.axis_index("col")
    x = lax.axis_index("row")
    z = col // 2
    core = lax.rem(col, 2)
    xr, xl = lax.rem(x + 1, nrow), lax.rem(x + nrow - 1, nrow)
    x2 = lax.rem(x + 2, nrow)
    up, down = lax.rem(col + 2, ncol), lax.rem(col + ncol - 2, ncol)
    mate = col + 1 - 2 * core
    home = z // per
    dist = lax.rem(x - home + nrow, nrow)
    lane0 = pl.multiple_of(lax.rem(z, per) * chip_wide, 128)

    def to(src, dst, ssem, rsem, **where):
        return pltpu.make_async_remote_copy(
            src_ref=src, dst_ref=dst, send_sem=ssem, recv_sem=rsem,
            device_id=where, device_id_type=MESH)

    own = pltpu.make_async_copy(pd, panel.at[col], own_s)
    own.start()
    small = [pltpu.make_async_copy(a, b, in_s.at[i])
             for i, (a, b) in enumerate((
                 (bands_in, bands), (wave_in, wave), (scale_in, scale), (valence_in, valence),
                 (conduction_in, conduction), (momentum_in, momentum)))]
    for copy in small:
        copy.start()
    barrier = pltpu.get_barrier_semaphore()
    for where in (dict(col=up), dict(col=down), dict(col=mate), dict(row=xr), dict(row=xl)):
        pl.semaphore_signal(barrier, inc=1, device_id=where, device_id_type=MESH)
    pl.semaphore_wait(barrier, 5)

    def chunk_of(d, s):
        away = jnp.where(d == 0, nz - s, s)
        return 2 * lax.rem(z + away, nz) + core

    def piece(ref, k, j):
        return ref.at[k, pl.ds(j * sub, sub)]

    def ring(d, s, j):
        k = chunk_of(d, s - 1)
        src = piece(panel, k, j)
        return to(src, piece(panel, k, j), ring_s.at[d, s - 1, j], ring_r.at[d, s - 1, j],
                  col=up if d == 0 else down)

    def ring_in(d, s, j):
        k = chunk_of(d, s)
        return to(piece(panel, k, j), piece(panel, k, j), ring_s.at[d, s - 1, j],
                  ring_r.at[d, s - 1, j], col=up)

    def pair(k, i, j):
        return to(piece(panel, k, j), piece(panel, k, j), pair_s.at[i, j], pair_r.at[i, j], col=mate)

    def cut(k, j):
        return panel.at[k, pl.ds(j * sub, sub), pl.ds(lane0, chip_wide)]

    def strip_first(k, i, j, side):
        return to(cut(k, j), piece(strip, k, j), sx_s.at[side, i, j], sx_r.at[i, j],
                  row=xr if side == 0 else xl)

    def strip_on(k, i, j, side):
        return to(piece(strip, k, j), piece(strip, k, j), sx_s.at[side, i, j], sx_r.at[i, j],
                  row=xr if side == 0 else xl)

    def strip_pair_first(k, i, j):
        return to(cut(k, j), piece(strip, k, j), sp_s.at[i, j], sp_r.at[i, j], col=mate)

    def strip_pair_on(k, i, j):
        return to(piece(strip, k, j), piece(strip, k, j), sp_s.at[i, j], sp_r.at[i, j], col=mate)

    def strip_local(k, i, j):
        return pltpu.make_async_copy(cut(k, j), piece(strip, k, j), loc_s.at[i, j])

    def place(d, s):
        return d * (half + 1) + s, chunk_of(d, s)

    def arrived(d, s, j):
        i, k = place(d, s)
        pair(k, i, j).start()

        @pl.when(dist == 0)
        def _():
            strip_first(k, i, j, 0).start()
            strip_first(k, i, j, 1).start()
            strip_pair_first(k, i, j).start()
            strip_local(k, i, j).start()

    def strip_step(d, s, j):
        i, k = place(d, s)

        @pl.when(dist != 0)
        def _():
            strip_on(k, i, j, 0).wait_recv()

        if d == 0:
            @pl.when(dist == 1)
            def _():
                strip_on(k, i, j, 0).start()
        else:
            @pl.when(dist == 3)
            def _():
                strip_on(k, i, j, 1).start()

        @pl.when(dist != 0)
        def _():
            strip_pair_on(k, i, j).start()

    def ready_panel(d, s, j):
        i, k = place(d, s)
        pair(k + 1 - 2 * core, i, j).wait_recv()

    def ready_strip(d, s, j):
        i, k = place(d, s)
        strip_pair_on(k + 1 - 2 * core, i, j).wait_recv()

        @pl.when(dist == 0)
        def _():
            strip_local(k, i, j).wait()

    def ready(d, s, j):
        ready_panel(d, s, j)
        ready_strip(d, s, j)

    def work(zi):
        spread(zi)
        gain(zi)

    def spread(zi):
        w0 = 2 * zi
        rows = 2 * ch
        wcol = weights[pl.ds(pl.multiple_of(w0 * ch, 8), rows)]
        for t in range(height // 128):
            lanes = slice(t * 128, (t + 1) * 128)
            pf = panel[pl.ds(w0, 2), :, lanes].reshape(rows, 128).astype(F32)
            wb = (pf * wcol).astype(BF)
            wpan[pl.ds(w0, 2), :, lanes] = wb.reshape(2, ch, 128)
            chir[:, lanes] += (wb.astype(F32) * pf).reshape(rows // 8, 8, 128).sum(0)

    def gain(zi):
        w0 = 2 * zi
        rows = 2 * ch
        wcol = weights[pl.ds(pl.multiple_of(w0 * ch, 8), rows)]
        for t in range(chip_wide // 128):
            lanes = slice(t * 128, (t + 1) * 128)
            sf = strip[pl.ds(w0, 2), :, lanes].reshape(rows, 128).astype(F32)
            wb = (sf * wcol).astype(BF).astype(F32)
            chic[:, lanes] += (wb * sf).reshape(rows // 8, 8, 128).sum(0)
        both = strip[pl.ds(w0, 2)].reshape(rows, chip_wide)
        mine = jnp.where(core == 0, both[:, :wide].astype(F32), both[:, wide:].astype(F32)).astype(BF)
        acc[...] += mm(mine, wpan[pl.ds(w0, 2)].reshape(rows, height), ((0,), (0,)))

    own.wait()
    for j in range(SUBS):
        ring(0, 1, j).start()
        ring(1, 1, j).start()
    for j in range(SUBS):
        arrived(0, 0, j)

    def subs_of(d, last):
        if not last:
            return range(SUBS)
        return range(SUBS // 2) if d == 0 else range(SUBS // 2, SUBS)

    def bring(s, last, final):
        for j in range(SUBS):
            for d in (0, 1):
                if j in subs_of(d, final):
                    ring_in(d, s, j).wait_recv()
                    if not final:
                        if j in subs_of(d, last):
                            ring(d, s + 1, j).start()
                    arrived(d, s, j)

    def relay(s, final):
        for j in range(SUBS):
            for d in (0, 1):
                if j in subs_of(d, final):
                    strip_step(d, s, j)

    def settle(s, final):
        for j in range(SUBS):
            for d in (0, 1):
                if j in subs_of(d, final):
                    ready(d, s, j)

    bring(1, False, False)
    acc[...] = jnp.zeros_like(acc)
    chir[...] = jnp.zeros_like(chir)
    chic[...] = jnp.zeros_like(chic)
    for copy in small:
        copy.wait()

    def look(ids, table):
        def level(v, found):
            return jnp.where(ids == v, table[v], found)
        return lax.fori_loop(0, table.shape[0], level, jnp.zeros(ids.shape, F32), unroll=4)

    tiles = weights.shape[0] // 128

    def stacked(i):
        return jnp.concatenate([bands[i:i + 1, t * 128:(t + 1) * 128] for t in range(tiles)], axis=0)

    weight = 4.0 / (look(stacked(0), valence) - look(stacked(1), conduction))
    for t in range(tiles):
        weights[t * 128:(t + 1) * 128] = jnp.broadcast_to(weight[t:t + 1], (128, 128)).T

    for j in range(SUBS):
        strip_step(0, 0, j)

    def early(s, carry):
        bring(s, False, False)
        relay(s - 1, False)

        @pl.when(s == 2)
        def _():
            for j in range(SUBS):
                ready(0, 0, j)

        @pl.when(s > 2)
        def _():
            settle(s - 2, False)

        def each(d, c):
            @pl.when((s > 2) | (d == 0))
            def _():
                work(chunk_of(d, s - 2) // 2)
            return c

        lax.fori_loop(0, 2, each, 0)
        return carry

    lax.fori_loop(2, half - 1, early, 0)
    def tail(s):
        settle(s, False)

        def each(d, c):
            work(chunk_of(d, s) // 2)
            return c
        lax.fori_loop(0, 2, each, 0)

    bring(half - 1, True, False)
    relay(half - 2, False)
    tail(half - 3)
    bring(half, False, True)
    relay(half - 1, False)
    tail(half - 2)

    @pl.when(dist != 2)
    def _():
        relay(half, True)

    tail(half - 1)
    far = chunk_of(0, half) // 2
    for d in (0, 1):
        for j in subs_of(d, True):
            ready_panel(d, half, j)
    spread(far)

    @pl.when(dist == 2)
    def _():
        relay(half, True)

    for d in (0, 1):
        for j in subs_of(d, True):
            ready_strip(d, half, j)
    gain(far)

    def root(first, count):
        lanes = pl.ds(pl.multiple_of(first, 128), count)
        total = jnp.zeros((1, count), F32)
        for i in range(3):
            shifted = wave[i:i + 1, lanes].astype(F32) + momentum[i]
            total = total + shifted * shifted
        return jnp.sqrt(4.0 * math.pi / total), scale[:, lanes]

    s_r, t_r = root(x * height, height)
    chi_r = jnp.sum(chir[...], axis=0, keepdims=True)
    diag_r = 1.0 - s_r * chi_r * s_r
    g_r = t_r / diag_r
    m_r = diag_r * g_r
    rvec[0:1] = g_r
    rvec[1:2] = g_r + (m_r.astype(BF).astype(F32) - m_r)
    rvec[2:3] = s_r * g_r
    rvec[3:4] = s_r
    s_l, t_l = root(z * chip_wide, chip_wide)
    chi_l = jnp.sum(chic[...], axis=0, keepdims=True)
    chic[0:1] = s_l
    chic[1:2] = t_l
    chic[2:3] = chi_l
    turned = chic[...].T
    turned = jnp.where(core == 0, turned[:wide], turned[wide:])
    s_c = turned[:, 0:1]
    diag_c = 1.0 - s_c * turned[:, 2:3] * s_c
    g_c = turned[:, 1:2] / diag_c
    alpha = (diag_c * g_c).astype(BF).astype(F32)
    cvec[:, 0:1] = g_c
    cvec[:, 1:2] = alpha
    cvec[:, 2:3] = s_c * g_c * alpha
    cvec[:, 3:4] = s_c * g_c * alpha * alpha
    cvec[:, 4:5] = s_c

    def js(h):
        return slice(h * hj, (h + 1) * hj)

    def same(h):
        rows = lax.broadcasted_iota(jnp.int32, (hj, height), 1) + x * height
        cols = lax.broadcasted_iota(jnp.int32, (hj, height), 0) + (col * wide + h * hj)
        return rows == cols

    def begin(h):
        ident = same(h)
        e = jnp.where(ident, 1.0, 0.0) - rvec[3:4] * acc[js(h)] * cvec[js(h), 4:5]
        eps_out[js(h)] = e
        m = (e * cvec[js(h), 0:1]).astype(BF)
        mixb[js(h)] = m
        rest = m.astype(F32) - jnp.where(ident, cvec[js(h), 1:2], 0.0)
        sbuf[js(h)] = (rest * rvec[2:3]).astype(BF)

    def product(h):
        return (rvec[1:2] * mixb[js(h)].astype(F32)) - rvec[3:4] * ybuf[js(h)]

    def middle(h):
        sq = product(h) - (rvec[3:4] * acc[js(h)]) * cvec[js(h), 2:3]
        square[js(h)] = sq
        m = sq.astype(BF)
        mixb[js(h)] = m
        a = cvec[js(h), 1:2]
        rest = m.astype(F32) - jnp.where(same(h), a * a, 0.0)
        sbuf[js(h)] = (rest * rvec[2:3]).astype(BF)

    def finish(h):
        cube = product(h) - (rvec[3:4] * acc[js(h)]) * cvec[js(h), 3:4]
        mixed = eps_out[js(h)] * cvec[js(h), 0:1]
        four = jnp.where(same(h), 4.0, 0.0)
        inv_out[js(h)] = rvec[0:1] * (four - 6.0 * mixed + 4.0 * square[js(h)] - cube)

    def q_part(h, q, d):
        rows = panel[pl.ds((2 * q + d) * cpp, cpp)].reshape(pp, height)
        return mm(sbuf[js(h)], rows, ((1,), (1,)))

    def hop(u, i, src, dst, right):
        return to(src, dst, x_s.at[u, i], x_r.at[u, i], row=xr if right else xl)

    def slot(u, i, right):
        return hop(u, i, qsend.at[u, i], qrecv.at[u, i], right)

    def quarter(u, q, d):
        return qfull.at[u, q, :, pl.ds(d * pp, pp)]

    def gathered(u, i, q, d, right):
        return hop(u, i, quarter(u, q, d), quarter(u, q, d), right)

    def stage1(u, h):
        for i, q, d, right in ((0, x2, 0, False), (1, x2, 1, True), (2, xl, 1, False), (3, xr, 0, True)):
            qsend[u, i] = q_part(h, q, d).astype(BF)
            slot(u, i, right).start()

    def kept(h, which):
        parts = ((0, xl, 0), (1, xr, 1)) if which == 0 else ((2, x, 0), (3, x, 1))
        for i, q, d in parts:
            keep[h, i] = q_part(h, q, d)

    def stage2(u, h):
        for i, right in ((0, False), (1, True)):
            slot(u, i, right).wait_recv()
            qsend[u, 4 + i] = (keep[h, i] + qrecv[u, i].astype(F32)).astype(BF)
            slot(u, 4 + i, right).start()

    def stage3(u, h):
        for i in (2, 3):
            slot(u, i, True).wait_recv()
        for d in (0, 1):
            slot(u, 4 + d, True).wait_recv()
            direct = qrecv[u, 3 - d].astype(F32)
            total = keep[h, 2 + d] + direct + qrecv[u, 4 + d].astype(F32)
            qfull[u, x, :, d * pp:(d + 1) * pp] = total.astype(BF)
            gathered(u, 6 + d, x, d, True).start()
            gathered(u, 8 + d, x, d, False).start()

    def add(u, h, q, first):
        term = mm(qfull[u, q], wpan[pl.ds(2 * q * cpp, 2 * cpp)].reshape(2 * pp, height), ((1,), (0,)))
        if first:
            ybuf[js(h)] = term
        else:
            ybuf[js(h)] += term

    def forward(u):
        gathered(u, 6, xl, 0, True).wait_recv()
        gathered(u, 10, xl, 0, True).start()
        gathered(u, 9, xr, 1, False).wait_recv()
        gathered(u, 11, xr, 1, False).start()

    def add_near(u, h):
        gathered(u, 7, xl, 1, True).wait_recv()
        add(u, h, xl, False)
        gathered(u, 8, xr, 0, False).wait_recv()
        add(u, h, xr, False)

    def add_far(u, h):
        gathered(u, 10, x2, 0, True).wait_recv()
        gathered(u, 11, x2, 1, False).wait_recv()
        add(u, h, x2, False)

    def exchange(u):
        stage2(u, 0)
        kept(1, 0)
        stage2(u + 1, 1)
        kept(0, 1)
        stage3(u, 0)
        kept(1, 1)
        stage3(u + 1, 1)
        add(u, 0, x, True)
        forward(u)
        add(u + 1, 1, x, True)
        add_near(u, 0)
        forward(u + 1)
        add_far(u, 0)

    begin(0)
    stage1(0, 0)
    begin(1)
    stage1(1, 1)
    kept(0, 0)
    exchange(0)
    middle(0)
    stage1(2, 0)
    add_near(1, 1)
    add_far(1, 1)
    middle(1)
    stage1(3, 1)
    kept(0, 0)
    exchange(2)
    finish(0)
    add_near(3, 1)
    add_far(3, 1)
    finish(1)

    for u in range(4):
        for i in range(6):
            slot(u, i, True).wait_send()
        for i in range(6, 12):
            gathered(u, i, x, 0, True).wait_send()

    def drain(d, s, j):
        i, k = place(d, s)
        pair(k, i, j).wait_send()
        strip_pair_on(k, i, j).wait_send()

        @pl.when((dist == 0) | (dist == (1 if d == 0 else 3)))
        def _():
            strip_on(k, i, j, d).wait_send()

        @pl.when(dist == 0)
        def _():
            strip_on(k, i, j, 1 - d).wait_send()

    for j in range(SUBS):
        drain(0, 0, j)

        def each(s, carry):
            for d in (0, 1):
                ring(d, s, j).wait_send()
                drain(d, s, j)
            return carry

        lax.fori_loop(1, half, each, 0)
        for d in (0, 1):
            if j in subs_of(d, True):
                ring(d, half, j).wait_send()
                drain(d, half, j)


def on_device(ncol, nrow, pair_density, band_pairs, valence, conduction, wave_vectors, momentum, guess_scale):
    ch, height = pair_density.shape
    pairs = ch * ncol
    wide = height * nrow // ncol
    scales = guess_scale[None, :]
    half = ncol // 4
    places = 2 * (half + 1)
    hj = wide // 2
    pp = pairs // 8
    vm = pl.BlockSpec(memory_space=pltpu.VMEM)
    hbm = pl.BlockSpec(memory_space=pltpu.HBM)
    dma = pltpu.SemaphoreType.DMA
    out = jax.ShapeDtypeStruct((wide, height), F32)
    eps_t, inv_t = pl.pallas_call(
        functools.partial(kernel, ncol, nrow),
        out_shape=(pltpu.VMEM((wide, height), F32), pltpu.VMEM((wide, height), F32)),
        in_specs=[hbm] * 7,
        out_specs=(vm, vm),
        scratch_shapes=[
            pltpu.VMEM(band_pairs.shape, jnp.int32),
            pltpu.VMEM(wave_vectors.shape, jnp.int32),
            pltpu.VMEM(scales.shape, F32),
            pltpu.SMEM(valence.shape, F32),
            pltpu.SMEM(conduction.shape, F32),
            pltpu.SMEM(momentum.shape, F32),
            pltpu.VMEM((pairs, 128), F32),
            pltpu.VMEM((ncol, ch, height), BF),
            pltpu.VMEM((ncol, ch, height), BF),
            pltpu.VMEM((ncol, ch, 2 * wide), BF),
            pltpu.VMEM((wide, height), F32),
            pltpu.VMEM((8, height), F32),
            pltpu.VMEM((8, 2 * wide), F32),
            pltpu.VMEM((8, height), F32),
            pltpu.VMEM((wide, 128), F32),
            pltpu.VMEM((wide, height), BF),
            pltpu.VMEM((wide, height), BF),
            pltpu.VMEM((wide, height), F32),
            pltpu.VMEM((wide, height), F32),
            pltpu.VMEM((2, 4, hj, pp), F32),
            pltpu.VMEM((4, 6, hj, pp), BF),
            pltpu.VMEM((4, 6, hj, pp), BF),
            pltpu.VMEM((4, nrow, hj, 2 * pp), BF),
            dma((6,)),
            dma((2, half, SUBS)),
            dma((2, half, SUBS)),
            dma((places, SUBS)),
            dma((places, SUBS)),
            dma((2, places, SUBS)),
            dma((places, SUBS)),
            dma((places, SUBS)),
            dma((places, SUBS)),
            dma(()),
            dma((places, SUBS)),
            dma((4, 12)),
            dma((4, 12)),
        ],
        compiler_params=pltpu.CompilerParams(
            collective_id=0, has_side_effects=True, vmem_limit_bytes=60 * 1024 * 1024
        ),
        name="cohsex",
    )(pair_density, band_pairs, wave_vectors, scales, valence, conduction, momentum)
    return eps_t.T, inv_t.T


def solution(mesh):
    placed = (P(("pb", "col"), "row"), P(), P(), P(), P(None, "pb"), P("pb"), P("pb"))
    return jax.shard_map(
        functools.partial(on_device, mesh.shape["col"], mesh.shape["row"]),
        mesh=mesh,
        in_specs=placed,
        out_specs=(P(("pb", "row"), "col"), P(("pb", "row"), "col")),
        check_vma=False,
    )
```

```python
import functools
import math

import jax
import jax.numpy as jnp
from jax import lax
from jax.experimental import pallas as pl
from jax.experimental.pallas import tpu as pltpu
from jax.sharding import PartitionSpec as P

MESH = pl.DeviceIdType.MESH
BF = jnp.bfloat16
F32 = jnp.float32
SUBS = 2


def mm(a, b, dims):
    return lax.dot_general(a, b, (dims, ((), ())), preferred_element_type=F32)


def kernel(ncol, nrow, pd, bands_in, wave_in, scale_in, valence_in, conduction_in, momentum_in,
           eps_out, inv_out,
           bands, wave, scale, valence, conduction, momentum, weights, panel, wpan, strip, acc, chir, chic, rvec, cvec, sbuf, mixb, square, ybuf,
           keep, qsend, qrecv, qfull,
           in_s, ring_s, ring_r, pair_s, pair_r, sx_s, sx_r, sp_s, sp_r, own_s, loc_s, x_s, x_r):
    nz = ncol // 2
    half = nz // 2
    per = nz // nrow
    ch, height = pd.shape
    sub = ch // SUBS
    chip_wide = strip.shape[2]
    wide = chip_wide // 2
    hj = wide // 2
    pp = keep.shape[3]
    cpp = pp // ch
    col = lax.axis_index("col")
    x = lax.axis_index("row")
    z = col // 2
    core = lax.rem(col, 2)
    xr, xl = lax.rem(x + 1, nrow), lax.rem(x + nrow - 1, nrow)
    x2 = lax.rem(x + 2, nrow)
    up, down = lax.rem(col + 2, ncol), lax.rem(col + ncol - 2, ncol)
    mate = col + 1 - 2 * core
    home = z // per
    dist = lax.rem(x - home + nrow, nrow)
    lane0 = pl.multiple_of(lax.rem(z, per) * chip_wide, 128)

    def to(src, dst, ssem, rsem, **where):
        return pltpu.make_async_remote_copy(
            src_ref=src, dst_ref=dst, send_sem=ssem, recv_sem=rsem,
            device_id=where, device_id_type=MESH)

    own = pltpu.make_async_copy(pd, panel.at[col], own_s)
    own.start()
    small = [pltpu.make_async_copy(a, b, in_s.at[i])
             for i, (a, b) in enumerate((
                 (bands_in, bands), (wave_in, wave), (scale_in, scale), (valence_in, valence),
                 (conduction_in, conduction), (momentum_in, momentum)))]
    for copy in small:
        copy.start()
    barrier = pltpu.get_barrier_semaphore()
    for where in (dict(col=up), dict(col=down), dict(col=mate), dict(row=xr), dict(row=xl)):
        pl.semaphore_signal(barrier, inc=1, device_id=where, device_id_type=MESH)
    pl.semaphore_wait(barrier, 5)

    def chunk_of(d, s):
        away = jnp.where(d == 0, nz - s, s)
        return 2 * lax.rem(z + away, nz) + core

    def piece(ref, k, j):
        return ref.at[k, pl.ds(j * sub, sub)]

    def ring(d, s, j):
        k = chunk_of(d, s - 1)
        src = piece(panel, k, j)
        return to(src, piece(panel, k, j), ring_s.at[d, s - 1, j], ring_r.at[d, s - 1, j],
                  col=up if d == 0 else down)

    def ring_in(d, s, j):
        k = chunk_of(d, s)
        return to(piece(panel, k, j), piece(panel, k, j), ring_s.at[d, s - 1, j],
                  ring_r.at[d, s - 1, j], col=up)

    def pair(k, i, j):
        return to(piece(panel, k, j), piece(panel, k, j), pair_s.at[i, j], pair_r.at[i, j], col=mate)

    def cut(k, j):
        return panel.at[k, pl.ds(j * sub, sub), pl.ds(lane0, chip_wide)]

    def strip_first(k, i, j, side):
        return to(cut(k, j), piece(strip, k, j), sx_s.at[side, i, j], sx_r.at[i, j],
                  row=xr if side == 0 else xl)

    def strip_on(k, i, j, side):
        return to(piece(strip, k, j), piece(strip, k, j), sx_s.at[side, i, j], sx_r.at[i, j],
                  row=xr if side == 0 else xl)

    def strip_pair_first(k, i, j):
        return to(cut(k, j), piece(strip, k, j), sp_s.at[i, j], sp_r.at[i, j], col=mate)

    def strip_pair_on(k, i, j):
        return to(piece(strip, k, j), piece(strip, k, j), sp_s.at[i, j], sp_r.at[i, j], col=mate)

    def strip_local(k, i, j):
        return pltpu.make_async_copy(cut(k, j), piece(strip, k, j), loc_s.at[i, j])

    def place(d, s):
        return d * (half + 1) + s, chunk_of(d, s)

    def arrived(d, s, j):
        i, k = place(d, s)
        pair(k, i, j).start()

        @pl.when(dist == 0)
        def _():
            strip_first(k, i, j, 0).start()
            strip_first(k, i, j, 1).start()
            strip_pair_first(k, i, j).start()
            strip_local(k, i, j).start()

    def strip_step(d, s, j):
        i, k = place(d, s)

        @pl.when(dist != 0)
        def _():
            strip_on(k, i, j, 0).wait_recv()

        if d == 0:
            @pl.when(dist == 1)
            def _():
                strip_on(k, i, j, 0).start()
        else:
            @pl.when(dist == 3)
            def _():
                strip_on(k, i, j, 1).start()

        @pl.when(dist != 0)
        def _():
            strip_pair_on(k, i, j).start()

    def ready_panel(d, s, j):
        i, k = place(d, s)
        pair(k + 1 - 2 * core, i, j).wait_recv()

    def ready_strip(d, s, j):
        i, k = place(d, s)
        strip_pair_on(k + 1 - 2 * core, i, j).wait_recv()

        @pl.when(dist == 0)
        def _():
            strip_local(k, i, j).wait()

    def ready(d, s, j):
        ready_panel(d, s, j)
        ready_strip(d, s, j)

    def work(zi):
        spread(zi)
        gain(zi)

    def spread(zi):
        w0 = 2 * zi
        rows = 2 * ch
        wcol = weights[pl.ds(pl.multiple_of(w0 * ch, 8), rows)]
        for t in range(height // 128):
            lanes = slice(t * 128, (t + 1) * 128)
            pf = panel[pl.ds(w0, 2), :, lanes].reshape(rows, 128).astype(F32)
            wb = (pf * wcol).astype(BF)
            wpan[pl.ds(w0, 2), :, lanes] = wb.reshape(2, ch, 128)
            chir[:, lanes] += (wb.astype(F32) * pf).reshape(rows // 8, 8, 128).sum(0)

    def gain(zi):
        w0 = 2 * zi
        rows = 2 * ch
        wcol = weights[pl.ds(pl.multiple_of(w0 * ch, 8), rows)]
        for t in range(chip_wide // 128):
            lanes = slice(t * 128, (t + 1) * 128)
            sf = strip[pl.ds(w0, 2), :, lanes].reshape(rows, 128).astype(F32)
            wb = (sf * wcol).astype(BF).astype(F32)
            chic[:, lanes] += (wb * sf).reshape(rows // 8, 8, 128).sum(0)
        both = strip[pl.ds(w0, 2)].reshape(rows, chip_wide)
        mine = jnp.where(core == 0, both[:, :wide].astype(F32), both[:, wide:].astype(F32)).astype(BF)
        acc[...] += mm(mine, wpan[pl.ds(w0, 2)].reshape(rows, height), ((0,), (0,)))

    own.wait()
    for j in range(SUBS):
        ring(0, 1, j).start()
        ring(1, 1, j).start()
    for j in range(SUBS):
        arrived(0, 0, j)

    def subs_of(d, last):
        if not last:
            return range(SUBS)
        return range(SUBS // 2) if d == 0 else range(SUBS // 2, SUBS)

    def bring(s, last, final):
        for j in range(SUBS):
            for d in (0, 1):
                if j in subs_of(d, final):
                    ring_in(d, s, j).wait_recv()
                    if not final:
                        if j in subs_of(d, last):
                            ring(d, s + 1, j).start()
                    arrived(d, s, j)

    def relay(s, final):
        for j in range(SUBS):
            for d in (0, 1):
                if j in subs_of(d, final):
                    strip_step(d, s, j)

    def settle(s, final):
        for j in range(SUBS):
            for d in (0, 1):
                if j in subs_of(d, final):
                    ready(d, s, j)

    bring(1, False, False)
    acc[...] = jnp.zeros_like(acc)
    chir[...] = jnp.zeros_like(chir)
    chic[...] = jnp.zeros_like(chic)
    for copy in small:
        copy.wait()

    def look(ids, table):
        def level(v, found):
            return jnp.where(ids == v, table[v], found)
        return lax.fori_loop(0, table.shape[0], level, jnp.zeros(ids.shape, F32), unroll=4)

    tiles = weights.shape[0] // 128

    def stacked(i):
        return jnp.concatenate([bands[i:i + 1, t * 128:(t + 1) * 128] for t in range(tiles)], axis=0)

    weight = 4.0 / (look(stacked(0), valence) - look(stacked(1), conduction))
    for t in range(tiles):
        weights[t * 128:(t + 1) * 128] = jnp.broadcast_to(weight[t:t + 1], (128, 128)).T

    for j in range(SUBS):
        strip_step(0, 0, j)

    def early(s, carry):
        bring(s, False, False)
        relay(s - 1, False)

        @pl.when(s == 2)
        def _():
            for j in range(SUBS):
                ready(0, 0, j)

        @pl.when(s > 2)
        def _():
            settle(s - 2, False)

        def each(d, c):
            @pl.when((s > 2) | (d == 0))
            def _():
                work(chunk_of(d, s - 2) // 2)
            return c

        lax.fori_loop(0, 2, each, 0)
        return carry

    lax.fori_loop(2, half - 1, early, 0)
    def tail(s):
        settle(s, False)

        def each(d, c):
            work(chunk_of(d, s) // 2)
            return c
        lax.fori_loop(0, 2, each, 0)

    bring(half - 1, True, False)
    relay(half - 2, False)
    tail(half - 3)
    bring(half, False, True)
    relay(half - 1, False)
    tail(half - 2)

    @pl.when(dist != 2)
    def _():
        relay(half, True)

    tail(half - 1)
    far = chunk_of(0, half) // 2
    for d in (0, 1):
        for j in subs_of(d, True):
            ready_panel(d, half, j)
    spread(far)

    @pl.when(dist == 2)
    def _():
        relay(half, True)

    for d in (0, 1):
        for j in subs_of(d, True):
            ready_strip(d, half, j)
    gain(far)

    def root(first, count):
        lanes = pl.ds(pl.multiple_of(first, 128), count)
        total = jnp.zeros((1, count), F32)
        for i in range(3):
            shifted = wave[i:i + 1, lanes].astype(F32) + momentum[i]
            total = total + shifted * shifted
        return jnp.sqrt(4.0 * math.pi / total), scale[:, lanes]

    s_r, t_r = root(x * height, height)
    chi_r = jnp.sum(chir[...], axis=0, keepdims=True)
    diag_r = 1.0 - s_r * chi_r * s_r
    g_r = t_r / diag_r
    m_r = diag_r * g_r
    rvec[0:1] = g_r
    rvec[1:2] = g_r + (m_r.astype(BF).astype(F32) - m_r)
    rvec[2:3] = s_r * g_r
    rvec[3:4] = s_r
    s_l, t_l = root(z * chip_wide, chip_wide)
    chi_l = jnp.sum(chic[...], axis=0, keepdims=True)
    chic[0:1] = s_l
    chic[1:2] = t_l
    chic[2:3] = chi_l
    turned = chic[...].T
    turned = jnp.where(core == 0, turned[:wide], turned[wide:])
    s_c = turned[:, 0:1]
    diag_c = 1.0 - s_c * turned[:, 2:3] * s_c
    g_c = turned[:, 1:2] / diag_c
    alpha = (diag_c * g_c).astype(BF).astype(F32)
    cvec[:, 0:1] = g_c
    cvec[:, 1:2] = alpha
    cvec[:, 2:3] = s_c * g_c * alpha
    cvec[:, 3:4] = s_c * g_c * alpha * alpha
    cvec[:, 4:5] = s_c

    def js(h):
        return slice(h * hj, (h + 1) * hj)

    def same(h):
        rows = lax.broadcasted_iota(jnp.int32, (hj, height), 1) + x * height
        cols = lax.broadcasted_iota(jnp.int32, (hj, height), 0) + (col * wide + h * hj)
        return rows == cols

    def begin(h):
        ident = same(h)
        e = jnp.where(ident, 1.0, 0.0) - rvec[3:4] * acc[js(h)] * cvec[js(h), 4:5]
        eps_out[js(h)] = e
        m = (e * cvec[js(h), 0:1]).astype(BF)
        mixb[js(h)] = m
        rest = m.astype(F32) - jnp.where(ident, cvec[js(h), 1:2], 0.0)
        sbuf[js(h)] = (rest * rvec[2:3]).astype(BF)

    def product(h):
        return (rvec[1:2] * mixb[js(h)].astype(F32)) - rvec[3:4] * ybuf[js(h)]

    def middle(h):
        sq = product(h) - (rvec[3:4] * acc[js(h)]) * cvec[js(h), 2:3]
        square[js(h)] = sq
        m = sq.astype(BF)
        mixb[js(h)] = m
        a = cvec[js(h), 1:2]
        rest = m.astype(F32) - jnp.where(same(h), a * a, 0.0)
        sbuf[js(h)] = (rest * rvec[2:3]).astype(BF)

    def finish(h):
        cube = product(h) - (rvec[3:4] * acc[js(h)]) * cvec[js(h), 3:4]
        mixed = eps_out[js(h)] * cvec[js(h), 0:1]
        four = jnp.where(same(h), 4.0, 0.0)
        inv_out[js(h)] = rvec[0:1] * (four - 6.0 * mixed + 4.0 * square[js(h)] - cube)

    def q_part(h, q, d):
        rows = panel[pl.ds((2 * q + d) * cpp, cpp)].reshape(pp, height)
        return mm(sbuf[js(h)], rows, ((1,), (1,)))

    def hop(u, i, src, dst, right):
        return to(src, dst, x_s.at[u, i], x_r.at[u, i], row=xr if right else xl)

    def slot(u, i, right):
        return hop(u, i, qsend.at[u, i], qrecv.at[u, i], right)

    def quarter(u, q, d):
        return qfull.at[u, q, :, pl.ds(d * pp, pp)]

    def gathered(u, i, q, d, right):
        return hop(u, i, quarter(u, q, d), quarter(u, q, d), right)

    def stage1(u, h):
        for i, q, d, right in ((0, x2, 0, False), (1, x2, 1, True), (2, xl, 1, False), (3, xr, 0, True)):
            qsend[u, i] = q_part(h, q, d).astype(BF)
            slot(u, i, right).start()

    def kept(h, which):
        parts = ((0, xl, 0), (1, xr, 1)) if which == 0 else ((2, x, 0), (3, x, 1))
        for i, q, d in parts:
            keep[h, i] = q_part(h, q, d)

    def stage2(u, h):
        for i, right in ((0, False), (1, True)):
            slot(u, i, right).wait_recv()
            qsend[u, 4 + i] = (keep[h, i] + qrecv[u, i].astype(F32)).astype(BF)
            slot(u, 4 + i, right).start()

    def stage3(u, h):
        for i in (2, 3):
            slot(u, i, True).wait_recv()
        for d in (0, 1):
            slot(u, 4 + d, True).wait_recv()
            direct = qrecv[u, 3 - d].astype(F32)
            total = keep[h, 2 + d] + direct + qrecv[u, 4 + d].astype(F32)
            qfull[u, x, :, d * pp:(d + 1) * pp] = total.astype(BF)
            gathered(u, 6 if d == 0 else 9, x, d, d == 0).start()
        gathered(u, 7, x, 1, True).start()
        gathered(u, 8, x, 0, False).start()

    def add(u, h, q, first):
        term = mm(qfull[u, q], wpan[pl.ds(2 * q * cpp, 2 * cpp)].reshape(2 * pp, height), ((1,), (0,)))
        if first:
            ybuf[js(h)] = term
        else:
            ybuf[js(h)] += term

    def forward(u):
        gathered(u, 6, xl, 0, True).wait_recv()
        gathered(u, 10, xl, 0, True).start()
        gathered(u, 9, xr, 1, False).wait_recv()
        gathered(u, 11, xr, 1, False).start()

    def add_near(u, h):
        gathered(u, 7, xl, 1, True).wait_recv()
        add(u, h, xl, False)
        gathered(u, 8, xr, 0, False).wait_recv()
        add(u, h, xr, False)

    def add_far(u, h):
        gathered(u, 10, x2, 0, True).wait_recv()
        gathered(u, 11, x2, 1, False).wait_recv()
        add(u, h, x2, False)

    def exchange(u):
        stage2(u, 0)
        kept(1, 0)
        stage2(u + 1, 1)
        kept(0, 1)
        stage3(u, 0)
        kept(1, 1)
        stage3(u + 1, 1)
        add(u, 0, x, True)
        forward(u)
        add(u + 1, 1, x, True)
        add_near(u, 0)
        forward(u + 1)
        add_far(u, 0)

    begin(0)
    stage1(0, 0)
    begin(1)
    stage1(1, 1)
    kept(0, 0)
    exchange(0)
    middle(0)
    stage1(2, 0)
    add_near(1, 1)
    add_far(1, 1)
    middle(1)
    stage1(3, 1)
    kept(0, 0)
    exchange(2)
    finish(0)
    add_near(3, 1)
    add_far(3, 1)
    finish(1)

    for u in range(4):
        for i in range(6):
            slot(u, i, True).wait_send()
        for i in range(6, 12):
            gathered(u, i, x, 0, True).wait_send()

    def drain(d, s, j):
        i, k = place(d, s)
        pair(k, i, j).wait_send()
        strip_pair_on(k, i, j).wait_send()

        @pl.when((dist == 0) | (dist == (1 if d == 0 else 3)))
        def _():
            strip_on(k, i, j, d).wait_send()

        @pl.when(dist == 0)
        def _():
            strip_on(k, i, j, 1 - d).wait_send()

    for j in range(SUBS):
        drain(0, 0, j)

        def each(s, carry):
            for d in (0, 1):
                ring(d, s, j).wait_send()
                drain(d, s, j)
            return carry

        lax.fori_loop(1, half, each, 0)
        for d in (0, 1):
            if j in subs_of(d, True):
                ring(d, half, j).wait_send()
                drain(d, half, j)


def on_device(ncol, nrow, pair_density, band_pairs, valence, conduction, wave_vectors, momentum, guess_scale):
    ch, height = pair_density.shape
    pairs = ch * ncol
    wide = height * nrow // ncol
    scales = guess_scale[None, :]
    half = ncol // 4
    places = 2 * (half + 1)
    hj = wide // 2
    pp = pairs // 8
    vm = pl.BlockSpec(memory_space=pltpu.VMEM)
    hbm = pl.BlockSpec(memory_space=pltpu.HBM)
    dma = pltpu.SemaphoreType.DMA
    out = jax.ShapeDtypeStruct((wide, height), F32)
    eps_t, inv_t = pl.pallas_call(
        functools.partial(kernel, ncol, nrow),
        out_shape=(pltpu.VMEM((wide, height), F32), pltpu.VMEM((wide, height), F32)),
        in_specs=[hbm] * 7,
        out_specs=(vm, vm),
        scratch_shapes=[
            pltpu.VMEM(band_pairs.shape, jnp.int32),
            pltpu.VMEM(wave_vectors.shape, jnp.int32),
            pltpu.VMEM(scales.shape, F32),
            pltpu.SMEM(valence.shape, F32),
            pltpu.SMEM(conduction.shape, F32),
            pltpu.SMEM(momentum.shape, F32),
            pltpu.VMEM((pairs, 128), F32),
            pltpu.VMEM((ncol, ch, height), BF),
            pltpu.VMEM((ncol, ch, height), BF),
            pltpu.VMEM((ncol, ch, 2 * wide), BF),
            pltpu.VMEM((wide, height), F32),
            pltpu.VMEM((8, height), F32),
            pltpu.VMEM((8, 2 * wide), F32),
            pltpu.VMEM((8, height), F32),
            pltpu.VMEM((wide, 128), F32),
            pltpu.VMEM((wide, height), BF),
            pltpu.VMEM((wide, height), BF),
            pltpu.VMEM((wide, height), F32),
            pltpu.VMEM((wide, height), F32),
            pltpu.VMEM((2, 4, hj, pp), F32),
            pltpu.VMEM((4, 6, hj, pp), BF),
            pltpu.VMEM((4, 6, hj, pp), BF),
            pltpu.VMEM((4, nrow, hj, 2 * pp), BF),
            dma((6,)),
            dma((2, half, SUBS)),
            dma((2, half, SUBS)),
            dma((places, SUBS)),
            dma((places, SUBS)),
            dma((2, places, SUBS)),
            dma((places, SUBS)),
            dma((places, SUBS)),
            dma((places, SUBS)),
            dma(()),
            dma((places, SUBS)),
            dma((4, 12)),
            dma((4, 12)),
        ],
        compiler_params=pltpu.CompilerParams(
            collective_id=0, has_side_effects=True, vmem_limit_bytes=60 * 1024 * 1024
        ),
        name="cohsex",
    )(pair_density, band_pairs, wave_vectors, scales, valence, conduction, momentum)
    return eps_t.T, inv_t.T


def solution(mesh):
    placed = (P(("pb", "col"), "row"), P(), P(), P(), P(None, "pb"), P("pb"), P("pb"))
    return jax.shard_map(
        functools.partial(on_device, mesh.shape["col"], mesh.shape["row"]),
        mesh=mesh,
        in_specs=placed,
        out_specs=(P(("pb", "row"), "col"), P(("pb", "row"), "col")),
        check_vma=False,
    )
```
